256 devices in a mesh: layer: 16 (over z_hi, x), rep: 16 (over z_lo, y, core).
Axes of the slice: x: 4, y: 4, z: 8 (z_hi: 4, z_lo: 2; z = z_hi * 2 + z_lo), core: 2. Of those that a mesh axis runs over, the one named last changes fastest.
Arguments:
- inverse_root: bfloat16 [128, 16, 128, 128], P('layer', 'rep'), may hold values from -0.625 to 0.625
- square_root: bfloat16 [128, 16, 128, 128], P('layer', 'rep'), may hold values from -0.625 to 0.625
- pattern: int32 [128, 16], P('layer', 'rep'), may hold values from 0 to 1, as said below
Outputs:
- inverse_next: bfloat16 [128, 16, 128, 128], P('layer', 'rep')
- square_next: bfloat16 [128, 16, 128, 128], P('layer', 'rep')
The draws below stay inside these ranges and needn't reach their ends.
Inputs may be any that keep to these rules, and one draw needn't show every extreme that they name: 1 marks a tile of the common pattern. Slot 8 is 1 in every block row, and slot w of block row i is 0 where i - 8 + w lies outside 0 to 127.
All inputs are finite; a program needn't handle non-finite values.
Results may differ from the reference program's by a relative error of at most 0.018.
Values may be sent and summed in bfloat16 or wider, within the bound.
A program may use at most 64 MiB of HBM per device.

```python
import jax
import jax.numpy as jnp
from jax import lax

TILE = 128
BAND = 16
HALF = 8
NB = 128
N_REP = 16


def draw_pattern(key, part):
    row_ids = jnp.arange(NB, dtype=jnp.int32)[:, None]
    slot_ids = jnp.arange(BAND, dtype=jnp.int32)[None, :]
    column = row_ids - HALF + slot_ids
    inside = (column >= 0) & (column < NB)
    key_level = jax.random.fold_in(key, 11)
    key_tiles = jax.random.fold_in(key, 23)
    fill_level = jax.random.randint(key_level, (NB, 1), 15, 90)
    tile_draws = jax.random.randint(key_tiles, (NB, BAND), 0, 100)
    chosen = (tile_draws < fill_level) | (slot_ids == HALF)
    return (inside & chosen).astype(jnp.int32)


def shard_levels(own_key, shape, shards, low, high):
    def one(position, shards_of):
        draws = jax.random.uniform(jax.random.fold_in(jax.random.fold_in(own_key, 6), position), (shards_of,), jnp.float32, low / len(shards), high / len(shards))
        return jnp.repeat(jnp.exp(draws), shape[position] // shards_of).reshape((-1,) + (1,) * (len(shape) - position - 1))

    level = one(*shards[0])
    for cut in shards[1:]:
        level = level * one(*cut)
    return level


def bell_draw(rng, shape, width, bound, pieces=(), kind=jnp.bfloat16):
    factor_of = shard_levels(rng, shape, pieces, -0.22, 0.18) if pieces else 1.0
    drawn = jax.random.normal(rng, shape, jnp.float32) * width * factor_of
    return jnp.minimum(jnp.maximum(drawn, -bound), bound).astype(kind)


def setup_inputs(seed: int = 0) -> dict:
    streams_of = jax.random.split(jax.random.key(seed), 4)
    return {
        "inverse_root": bell_draw(streams_of[0], (NB, BAND, TILE, TILE), 0.1, 0.625, ((0, 16), (1, 16))),
        "square_root": bell_draw(streams_of[1], (NB, BAND, TILE, TILE), 0.1, 0.625, ((0, 16), (1, 16))),
        "pattern": draw_pattern(jax.random.fold_in(streams_of[3], 71), 0),
    }


def band_product(left_tiles, right_tiles):
    block_rows = left_tiles.shape[0]
    band_slots = left_tiles.shape[1]
    half_band = band_slots // 2
    group_slots = band_slots // N_REP
    padded = jnp.pad(right_tiles, ((half_band, half_band), (band_slots, band_slots), (0, 0), (0, 0)))
    total = jnp.zeros(left_tiles.shape, jnp.float32)
    for group in range(N_REP):
        partial_value = jnp.zeros(left_tiles.shape, jnp.float32)
        for inner in range(group * group_slots, (group + 1) * group_slots):
            low_slot = max(0, inner - half_band)
            high_slot = min(band_slots, inner + half_band)
            offset = band_slots + half_band - inner
            shifted = padded[inner:inner + block_rows, offset + low_slot:offset + high_slot]
            product = jnp.einsum("iab,iwbc->iwac", left_tiles[:, inner].astype(jnp.float32), shifted.astype(jnp.float32))
            partial_value = partial_value.at[:, low_slot:high_slot].add(product)
        rounded = lax.optimization_barrier(partial_value.astype(jnp.bfloat16))
        total = total + rounded.astype(jnp.float32)
    return total


def reference(inverse_root, square_root, pattern):
    in_pattern = (pattern == 1)[:, :, None, None]
    inverse_kept = jnp.where(in_pattern, inverse_root, jnp.zeros_like(inverse_root))
    square_kept = jnp.where(in_pattern, square_root, jnp.zeros_like(square_root))
    intersection = jnp.where(in_pattern, band_product(inverse_kept, square_kept), jnp.float32(0.0))
    band_slots = pattern.shape[1]
    half_band = band_slots // 2
    diagonal = (jnp.arange(band_slots, dtype=jnp.int32) == half_band).astype(jnp.float32)
    identity = jnp.eye(inverse_root.shape[2], dtype=jnp.float32)
    update = jnp.where(in_pattern, 1.5 * diagonal[None, :, None, None] * identity - 0.5 * intersection, jnp.float32(0.0)).astype(jnp.bfloat16)
    square_next = jnp.where(in_pattern, band_product(square_kept, update), jnp.float32(0.0)).astype(jnp.bfloat16)
    inverse_next = jnp.where(in_pattern, band_product(update, inverse_kept), jnp.float32(0.0)).astype(jnp.bfloat16)
    return inverse_next, square_next
```

```python
import functools

import jax
import jax.numpy as jnp
from jax import lax
from jax.experimental import pallas as pl
from jax.experimental.pallas import tpu as pltpu
from jax.sharding import PartitionSpec as P

BF = jnp.bfloat16
F32 = jnp.float32
MESH = pl.DeviceIdType.MESH
Z, Y, U = 0, 1, 2


def mod(a, b):
    return lax.rem(a, jnp.int32(b))


def div(a, b):
    return lax.div(a, jnp.int32(b))


def kernel(
    layers, t,
    z_hbm, y_hbm, pat_ref, w_out, x_out,
    raw, kept, marks, marks_home, left, right, lhs, rhs, prod, give, got, done, land,
    in_sem, home_send, home_recv, mark_send, mark_recv,
    left_send, left_recv, right_send, right_recv, pair_send, pair_recv, out_send, out_recv,
):
    l = lax.axis_index("layer")
    r = lax.axis_index("rep")
    h, y, c = div(r, 8), mod(div(r, 2), 4), mod(r, 2)
    big = 2 * l + h
    shift = 8 * mod(l + 1, 2)
    delta = mod(y + 4 * layers * 2 - big, 4)
    other = 1 - c
    pending = []

    def rep_of(hh, yy, cc):
        return hh * 8 + yy * 2 + cc

    def remote(src, dst, send_sem, recv_sem, layer, rep, cond=None):
        copy = pltpu.make_async_remote_copy(
            src_ref=src, dst_ref=dst, send_sem=send_sem, recv_sem=recv_sem,
            device_id=(layer, rep), device_id_type=MESH,
        )
        if cond is None:
            copy.start()
        else:
            pl.when(cond)(copy.start)
        pending.append((cond, copy))

    def arrive(dst, recv_sem, cond=None):
        copy = pltpu.make_async_remote_copy(
            src_ref=dst, dst_ref=dst, send_sem=recv_sem, recv_sem=recv_sem,
            device_id=(l, r), device_id_type=MESH,
        )
        if cond is None:
            copy.wait_recv()
        else:
            pl.when(cond)(copy.wait_recv)

    loads = [
        pltpu.make_async_copy(ref.at[:, 0], raw.at[k], in_sem.at[k])
        for k, ref in ((Z, z_hbm), (Y, y_hbm))
    ]
    for load in loads:
        load.start()

    barrier = pltpu.get_barrier_semaphore()
    for step in range(1, 16):
        pl.semaphore_signal(
            barrier, inc=1, device_id=(l, mod(r + step, 16)), device_id_type=MESH
        )
    for near in (mod(l + 1, layers), mod(l + layers - 1, layers)):
        for hh in range(2):
            for cc in range(2):
                pl.semaphore_signal(
                    barrier, inc=1, device_id=(near, rep_of(hh, y, cc)), device_id_type=MESH
                )

    for ap in range(8):
        marks[ap] = jnp.full((8, 128), pat_ref[ap, 0], jnp.int32)
    for k in (Z, Y):
        loads[k].wait()
        for ap in range(8):
            kept[k, ap] = jnp.where(pat_ref[ap, 0] == 1, raw[k, ap], jnp.zeros((t, t), BF))
    pl.semaphore_wait(barrier, 23)

    def scatter(k):
        for ap in range(8):
            jm = mod(shift + ap + r, 16)
            yd, cd, b2 = div(jm, 4), div(mod(jm, 4), 2), mod(jm, 2)
            dest = rep_of(ap // 4, yd, cd)
            here, away = dest == r, dest != r
            a = ap % 4

            @pl.when(here)
            def _():
                left[k, yd, a, b2] = kept[k, ap]
                if k == Y:
                    marks_home[a, b2] = marks[ap]

            remote(
                kept.at[k, ap], left.at[k, yd, a, b2], home_send.at[k, ap],
                home_recv.at[k, a, b2], l, dest, away,
            )
            if k == Y:
                remote(
                    marks.at[ap], marks_home.at[a, b2], mark_send.at[ap],
                    mark_recv.at[a, b2], l, dest, away,
                )

    def from_other(a, b2):
        source = mod(4 * y + 2 * c + b2 - shift - (4 * h + a) + 32, 16)
        return source != r

    def home_ready(k):
        for a in range(4):
            for b2 in range(2):
                arrive(left.at[k, y, a, b2], home_recv.at[k, a, b2], from_other(a, b2))

    up, down = mod(y + 1, 4), mod(y + 3, 4)
    far = mod(y + 2, 4)

    def left_start(k):
        for step, half in ((0, 0), (1, 1)):
            part = pl.ds(2 * half, 2)
            remote(
                left.at[k, y, part], left.at[k, y, part], left_send.at[k, half],
                left_recv.at[k, half], l, rep_of(h, up, c),
            )
            back = 1 - half
            part = pl.ds(2 * back, 2)
            remote(
                left.at[k, y, part], left.at[k, y, part], left_send.at[k, 2 + back],
                left_recv.at[k, 2 + back], l, rep_of(h, down, c),
            )

    def left_forward(k):
        arrive(left.at[k, down, pl.ds(0, 2)], left_recv.at[k, 0])
        remote(
            left.at[k, down, pl.ds(0, 2)], left.at[k, down, pl.ds(0, 2)], left_send.at[k, 4],
            left_recv.at[k, 4], l, rep_of(h, up, c),
        )
        arrive(left.at[k, up, pl.ds(2, 2)], left_recv.at[k, 3])
        remote(
            left.at[k, up, pl.ds(2, 2)], left.at[k, up, pl.ds(2, 2)], left_send.at[k, 5],
            left_recv.at[k, 5], l, rep_of(h, down, c),
        )

    def left_ready(k):
        arrive(left.at[k, down, pl.ds(2, 2)], left_recv.at[k, 1])
        arrive(left.at[k, up, pl.ds(0, 2)], left_recv.at[k, 2])
        arrive(left.at[k, far, pl.ds(0, 2)], left_recv.at[k, 4])
        arrive(left.at[k, far, pl.ds(2, 2)], left_recv.at[k, 5])

    def right_start(k):
        for d in (2, -2, 1, -1):
            there = mod(big + d + 2 * layers, 2 * layers)
            ld, hd = div(there, 2), mod(there, 2)
            cond = None
            if d == 2:
                cond = mod(delta + 4 - d, 4) != 1
            if d == -2:
                cond = mod(delta + 4 - d, 4) != 3
            for cd in range(2):
                remote(
                    left.at[k, y, pl.ds(2 * cd, 2)], right.at[k, 2 - d, c],
                    right_send.at[k, 2 - d, cd], right_recv.at[k, 2 - d, c],
                    ld, rep_of(hd, y, cd), cond,
                )
        remote(
            left.at[k, y, pl.ds(2 * other, 2)], right.at[k, 2, c],
            right_send.at[k, 2, 0], right_recv.at[k, 2, c], l, rep_of(h, y, other),
        )
        right[k, 2, c] = left[k, y, pl.ds(2 * c, 2)]

    def right_ready(k):
        arrive(right.at[k, 2, other], right_recv.at[k, 2, other])
        for n in (1, 3, 0, 4):
            cond = None
            if n == 0:
                cond = delta != 1
            if n == 4:
                cond = delta != 3
            for cc in range(2):
                arrive(right.at[k, n, cc], right_recv.at[k, n, cc], cond)

    nothing = jnp.zeros((t, t), BF)
    apart = delta == 2
    toward = jnp.where(delta == 3, -1, delta)
    middle = (jnp.where(apart, -2, toward), jnp.where(apart, 2, toward))

    def multiply(kl, kr):
        for s in range(2):
            for at, n in enumerate((0, 1, 2) if s == 0 else (2, 3, 4)):
                cls = mod(big + n + 2, 4)
                gap = middle[s] - (n - 2)
                for kk in range(2):
                    inner = 2 * c + kk
                    for a in range(4):
                        tile = left[kl, cls, a, kk]
                        if n == 0:
                            tile = jnp.where(inner >= a, tile, nothing)
                        if n == 4:
                            tile = jnp.where(inner < a, tile, nothing)
                        lhs[s, a * t:(a + 1) * t, (2 * at + kk) * t:(2 * at + kk + 1) * t] = tile
                    for b in range(4):
                        whole = jnp.logical_and(gap >= -1, gap <= 1)
                        low = jnp.logical_and(gap == 2, b < inner)
                        high = jnp.logical_and(gap == -2, b >= inner)
                        good = jnp.logical_or(whole, jnp.logical_or(low, high))
                        if s == 1 and n == 2:
                            good = jnp.logical_and(good, apart)
                        tile = jnp.where(good, right[kr, n, b // 2, kk, b % 2], nothing)
                        rhs[s, (2 * at + kk) * t:(2 * at + kk + 1) * t, b * t:(b + 1) * t] = tile
        for s in range(2):
            for half in range(2):
                out = jnp.dot(
                    lhs[s], rhs[s, :, half * 2 * t:(half + 1) * 2 * t], preferred_element_type=F32
                )
                for a in range(4):
                    for b2 in range(2):
                        prod[s, a, 2 * half + b2] = out[a * t:(a + 1) * t, b2 * t:(b2 + 1) * t]

    def total(a, b):
        first = jnp.logical_or(jnp.logical_not(apart), b >= a)
        second = jnp.logical_or(jnp.logical_not(apart), b < a)
        empty = jnp.zeros((t, t), F32)
        return jnp.where(first, prod[0, a, b], empty) + jnp.where(second, prod[1, a, b], empty)

    def share(k):
        for a in range(4):
            for b2 in range(2):
                give[k, a, b2] = total(a, 2 * other + b2).astype(BF)
                prod[0, a, 2 * c + b2] = total(a, 2 * c + b2)
        remote(
            give.at[k], got.at[k], pair_send.at[k], pair_recv.at[k], l, rep_of(h, y, other)
        )

    def summed(k, a, b2):
        value = prod[0, a, 2 * c + b2] + got[k, a, b2].astype(F32)
        return value

    def marked(a, b2):
        return marks_home[a, b2][0:1, :] == 1

    def owner_send(k):
        for a in range(4):
            for b2 in range(2):
                slot = mod(4 * y + 2 * c + b2 + shift - (4 * h + a) + 32, 16)
                done[k, a, b2] = jnp.where(
                    marked(a, b2), summed(k, a, b2), jnp.zeros((t, t), F32)
                ).astype(BF)
        for a in range(4):
            for b2 in range(2):
                slot = mod(4 * y + 2 * c + b2 + shift - (4 * h + a) + 32, 16)
                here, away = slot == r, slot != r

                @pl.when(here)
                def _():
                    land[k, 4 * h + a] = done[k, a, b2]

                remote(
                    done.at[k, a, b2], land.at[k, 4 * h + a], out_send.at[k, a, b2],
                    out_recv.at[k, 4 * h + a], l, slot, away,
                )

    def owner_ready(k, out_ref):
        for ap in range(8):
            jm = mod(shift + ap + r, 16)
            source = rep_of(ap // 4, div(jm, 4), div(mod(jm, 4), 2))
            arrive(land.at[k, ap], out_recv.at[k, ap], source != r)
        for ap in range(8):
            out_ref[ap, 0] = land[k, ap]

    scatter(Y)
    scatter(Z)
    home_ready(Y)
    right_start(Y)
    home_ready(Z)
    left_start(Z)
    right_start(Z)
    left_forward(Z)
    left_start(Y)
    for a in range(4):
        for b2 in range(2):
            arrive(marks_home.at[a, b2], mark_recv.at[a, b2], from_other(a, b2))
    left_ready(Z)
    right_ready(Y)
    multiply(Z, Y)
    share(U)
    left_forward(Y)
    arrive(got.at[U], pair_recv.at[U])
    rows = lax.broadcasted_iota(jnp.int32, (t, t), 0)
    cols = lax.broadcasted_iota(jnp.int32, (t, t), 1)
    for a in range(4):
        for b2 in range(2):
            on = jnp.logical_and(mod(big, 4) == y, 2 * c + b2 == a)
            eye = jnp.where(rows == cols, jnp.where(on, F32(1.5), F32(0.0)), F32(0.0))
            value = eye - 0.5 * summed(U, a, b2)
            left[U, y, a, b2] = jnp.where(marked(a, b2), value, jnp.zeros((t, t), F32)).astype(BF)
    left_start(U)
    right_start(U)
    left_forward(U)
    right_ready(Z)
    left_ready(U)
    multiply(U, Z)
    share(Z)
    arrive(got.at[Z], pair_recv.at[Z])
    owner_send(Z)
    left_ready(Y)
    right_ready(U)
    multiply(Y, U)
    share(Y)
    arrive(got.at[Y], pair_recv.at[Y])
    owner_send(Y)
    owner_ready(Z, w_out)
    owner_ready(Y, x_out)
    for cond, copy in pending:
        if cond is None:
            copy.wait_send()
        else:
            pl.when(cond)(copy.wait_send)


def solution(mesh):
    layers = mesh.shape["layer"]

    def body(inverse_root, square_root, pattern):
        t = inverse_root.shape[-1]
        dma = pltpu.SemaphoreType.DMA
        return pl.pallas_call(
            functools.partial(kernel, layers, t),
            out_shape=[
                jax.ShapeDtypeStruct(inverse_root.shape, BF),
                jax.ShapeDtypeStruct(square_root.shape, BF),
            ],
            in_specs=[
                pl.BlockSpec(memory_space=pl.ANY),
                pl.BlockSpec(memory_space=pl.ANY),
                pl.BlockSpec(memory_space=pltpu.SMEM),
            ],
            out_specs=[pl.BlockSpec(memory_space=pltpu.VMEM)] * 2,
            scratch_shapes=[
                pltpu.VMEM((2, 8, t, t), BF),
                pltpu.VMEM((2, 8, t, t), BF),
                pltpu.VMEM((8, 8, 128), jnp.int32),
                pltpu.VMEM((4, 2, 8, 128), jnp.int32),
                pltpu.VMEM((3, 4, 4, 2, t, t), BF),
                pltpu.VMEM((3, 5, 2, 2, 2, t, t), BF),
                pltpu.VMEM((2, 4 * t, 6 * t), BF),
                pltpu.VMEM((2, 6 * t, 4 * t), BF),
                pltpu.VMEM((2, 4, 4, t, t), F32),
                pltpu.VMEM((3, 4, 2, t, t), BF),
                pltpu.VMEM((3, 4, 2, t, t), BF),
                pltpu.VMEM((2, 4, 2, t, t), BF),
                pltpu.VMEM((2, 8, t, t), BF),
                dma((2,)),
                dma((2, 8)),
                dma((2, 4, 2)),
                dma((8,)),
                dma((4, 2)),
                dma((3, 6)),
                dma((3, 6)),
                dma((3, 5, 2)),
                dma((3, 5, 2)),
                dma((3,)),
                dma((3,)),
                dma((2, 4, 2)),
                dma((2, 8)),
            ],
            compiler_params=pltpu.CompilerParams(
                collective_id=0, has_side_effects=True, vmem_limit_bytes=40 * 1024 * 1024
            ),
            name="band_step",
        )(inverse_root, square_root, pattern)

    return jax.shard_map(
        body,
        mesh=mesh,
        in_specs=(P("layer", "rep", None, None), P("layer", "rep", None, None), P("layer", "rep")),
        out_specs=(P("layer", "rep", None, None), P("layer", "rep", None, None)),
        check_vma=False,
    )
```

```python
import functools

import jax
import jax.numpy as jnp
from jax import lax
from jax.experimental import pallas as pl
from jax.experimental.pallas import tpu as pltpu
from jax.sharding import PartitionSpec as P

BF = jnp.bfloat16
F32 = jnp.float32
MESH = pl.DeviceIdType.MESH
Z, Y, U = 0, 1, 2


def mod(a, b):
    return lax.rem(a, jnp.int32(b))


def div(a, b):
    return lax.div(a, jnp.int32(b))


def kernel(
    layers, t,
    z_hbm, y_hbm, pat_ref, w_out, x_out,
    raw, kept, marks, marks_home, left, right, lhs, rhs, prod, give, got, done, land,
    in_sem, home_send, home_recv, mark_send, mark_recv,
    left_send, left_recv, right_send, right_recv, relay_send, pair_send, pair_recv, out_send, out_recv,
):
    l = lax.axis_index("layer")
    r = lax.axis_index("rep")
    h, y, c = div(r, 8), mod(div(r, 2), 4), mod(r, 2)
    big = 2 * l + h
    shift = 8 * mod(l + 1, 2)
    delta = mod(y + 4 * layers * 2 - big, 4)
    other = 1 - c
    pending = []

    def rep_of(hh, yy, cc):
        return hh * 8 + yy * 2 + cc

    def remote(src, dst, send_sem, recv_sem, layer, rep, cond=None):
        copy = pltpu.make_async_remote_copy(
            src_ref=src, dst_ref=dst, send_sem=send_sem, recv_sem=recv_sem,
            device_id=(layer, rep), device_id_type=MESH,
        )
        if cond is None:
            copy.start()
        else:
            pl.when(cond)(copy.start)
        pending.append((cond, copy))

    def arrive(dst, recv_sem, cond=None):
        copy = pltpu.make_async_remote_copy(
            src_ref=dst, dst_ref=dst, send_sem=recv_sem, recv_sem=recv_sem,
            device_id=(l, r), device_id_type=MESH,
        )
        if cond is None:
            copy.wait_recv()
        else:
            pl.when(cond)(copy.wait_recv)

    loads = [
        pltpu.make_async_copy(ref.at[:, 0], raw.at[k], in_sem.at[k])
        for k, ref in ((Z, z_hbm), (Y, y_hbm))
    ]
    for load in loads:
        load.start()

    barrier = pltpu.get_barrier_semaphore()
    for step in range(1, 16):
        pl.semaphore_signal(
            barrier, inc=1, device_id=(l, mod(r + step, 16)), device_id_type=MESH
        )
    above, below = l < layers - 1, l > 0
    for near, there in ((l + 1, above), (l - 1, below)):

        @pl.when(there)
        def _():
            for hh in range(2):
                for cc in range(2):
                    pl.semaphore_signal(
                        barrier, inc=1, device_id=(near, rep_of(hh, y, cc)), device_id_type=MESH
                    )


    for ap in range(8):
        marks[ap] = jnp.full((8, 128), pat_ref[ap, 0], jnp.int32)
    for k in (Z, Y):
        loads[k].wait()
        for ap in range(8):
            kept[k, ap] = jnp.where(pat_ref[ap, 0] == 1, raw[k, ap], jnp.zeros((t, t), BF))
    peers = 15 + 4 * (above.astype(jnp.int32) + below.astype(jnp.int32))
    pl.semaphore_wait(barrier, peers)

    def scatter(k):
        for ap in range(8):
            jm = mod(shift + ap + r, 16)
            yd, cd, b2 = div(jm, 4), div(mod(jm, 4), 2), mod(jm, 2)
            dest = rep_of(ap // 4, yd, cd)
            here, away = dest == r, dest != r
            a = ap % 4

            @pl.when(here)
            def _():
                left[k, yd, a, b2] = kept[k, ap]
                if k == Y:
                    marks_home[a, b2] = marks[ap]

            remote(
                kept.at[k, ap], left.at[k, yd, a, b2], home_send.at[k, ap],
                home_recv.at[k, a, b2], l, dest, away,
            )
            if k == Y:
                remote(
                    marks.at[ap], marks_home.at[a, b2], mark_send.at[ap],
                    mark_recv.at[a, b2], l, dest, away,
                )

    def from_other(a, b2):
        source = mod(4 * y + 2 * c + b2 - shift - (4 * h + a) + 32, 16)
        return source != r

    def home_ready(k):
        for a in range(4):
            for b2 in range(2):
                arrive(left.at[k, y, a, b2], home_recv.at[k, a, b2], from_other(a, b2))

    up, down = mod(y + 1, 4), mod(y + 3, 4)
    far = mod(y + 2, 4)

    def left_start(k):
        for step, half in ((0, 0), (1, 1)):
            part = pl.ds(2 * half, 2)
            remote(
                left.at[k, y, part], left.at[k, y, part], left_send.at[k, half],
                left_recv.at[k, half], l, rep_of(h, up, c),
            )
            back = 1 - half
            part = pl.ds(2 * back, 2)
            remote(
                left.at[k, y, part], left.at[k, y, part], left_send.at[k, 2 + back],
                left_recv.at[k, 2 + back], l, rep_of(h, down, c),
            )

    def left_forward(k):
        arrive(left.at[k, down, pl.ds(0, 2)], left_recv.at[k, 0])
        remote(
            left.at[k, down, pl.ds(0, 2)], left.at[k, down, pl.ds(0, 2)], left_send.at[k, 4],
            left_recv.at[k, 4], l, rep_of(h, up, c),
        )
        arrive(left.at[k, up, pl.ds(2, 2)], left_recv.at[k, 3])
        remote(
            left.at[k, up, pl.ds(2, 2)], left.at[k, up, pl.ds(2, 2)], left_send.at[k, 5],
            left_recv.at[k, 5], l, rep_of(h, down, c),
        )

    def left_ready(k):
        arrive(left.at[k, down, pl.ds(2, 2)], left_recv.at[k, 1])
        arrive(left.at[k, up, pl.ds(0, 2)], left_recv.at[k, 2])
        arrive(left.at[k, far, pl.ds(0, 2)], left_recv.at[k, 4])
        arrive(left.at[k, far, pl.ds(2, 2)], left_recv.at[k, 5])

    first, last = h == 0, h == 1
    edge_up, edge_down = mod(l, 4) == 3, mod(l, 4) == 0
    both = jnp.logical_and

    def inside(n):
        row = big + n - 2
        return both(row >= 0, row < 2 * layers)

    def wanted(n, dl):
        if n == 0:
            return dl != 1
        if n == 4:
            return dl != 3
        return None

    def needed(n):
        cond = inside(n)
        want = wanted(n, delta)
        return cond if want is None else both(cond, want)

    def right_start(k):
        for d in (2, -2, 1, -1):
            there = big + d
            ld, hd = div(there, 2), mod(there, 2)
            cond = both(there >= 0, there < 2 * layers)
            want = wanted(2 - d, mod(delta + 4 - d, 4))
            if want is not None:
                cond = both(cond, want)
            if d == 2:
                cond = both(cond, jnp.logical_not(both(last, edge_up)))
            if d == -2:
                cond = both(cond, jnp.logical_not(both(first, edge_down)))
            for cd in range(2):
                remote(
                    left.at[k, y, pl.ds(2 * cd, 2)], right.at[k, 2 - d, c],
                    right_send.at[k, 2 - d, cd], right_recv.at[k, 2 - d, c],
                    ld, rep_of(hd, y, cd), cond,
                )
        remote(
            left.at[k, y, pl.ds(2 * other, 2)], right.at[k, 2, c],
            right_send.at[k, 2, 0], right_recv.at[k, 2, c], l, rep_of(h, y, other),
        )
        right[k, 2, c] = left[k, y, pl.ds(2 * c, 2)]

    def right_relay(k):
        for src, dst, side, step in ((1, 0, both(first, both(edge_down, below)), 3),
                                     (3, 4, both(last, both(edge_up, above)), 1)):
            for cc in range(2):
                arrive(right.at[k, src, cc], right_recv.at[k, src, cc], side)
                remote(
                    right.at[k, src, cc], right.at[k, dst, cc], relay_send.at[k, cc],
                    right_recv.at[k, dst, cc], l, rep_of(1 - h, y, c),
                    both(side, wanted(dst, mod(delta + step, 4))),
                )

    def right_ready(k):
        arrive(right.at[k, 2, other], right_recv.at[k, 2, other])
        for n in (1, 3, 0, 4):
            cond = needed(n)
            if n == 1:
                cond = both(cond, jnp.logical_not(both(first, edge_down)))
            if n == 3:
                cond = both(cond, jnp.logical_not(both(last, edge_up)))
            for cc in range(2):
                arrive(right.at[k, n, cc], right_recv.at[k, n, cc], cond)

    nothing = jnp.zeros((t, t), BF)
    apart = delta == 2
    toward = jnp.where(delta == 3, -1, delta)
    middle = (jnp.where(apart, -2, toward), jnp.where(apart, 2, toward))

    def multiply(kl, kr):
        for s in range(2):
            for at, n in enumerate((0, 1, 2) if s == 0 else (2, 3, 4)):
                cls = mod(big + n + 2, 4)
                gap = middle[s] - (n - 2)
                for kk in range(2):
                    inner = 2 * c + kk
                    for a in range(4):
                        tile = left[kl, cls, a, kk]
                        if n == 0:
                            tile = jnp.where(inner >= a, tile, nothing)
                        if n == 4:
                            tile = jnp.where(inner < a, tile, nothing)
                        lhs[s, a * t:(a + 1) * t, (2 * at + kk) * t:(2 * at + kk + 1) * t] = tile
                    for b in range(4):
                        whole = jnp.logical_and(gap >= -1, gap <= 1)
                        low = jnp.logical_and(gap == 2, b < inner)
                        high = jnp.logical_and(gap == -2, b >= inner)
                        good = jnp.logical_or(whole, jnp.logical_or(low, high))
                        if n != 2:
                            good = both(good, inside(n))
                        if s == 1 and n == 2:
                            good = jnp.logical_and(good, apart)
                        tile = jnp.where(good, right[kr, n, b // 2, kk, b % 2], nothing)
                        rhs[s, (2 * at + kk) * t:(2 * at + kk + 1) * t, b * t:(b + 1) * t] = tile
        for s in range(2):
            for half in range(2):
                out = jnp.dot(
                    lhs[s], rhs[s, :, half * 2 * t:(half + 1) * 2 * t], preferred_element_type=F32
                )
                for a in range(4):
                    for b2 in range(2):
                        prod[s, a, 2 * half + b2] = out[a * t:(a + 1) * t, b2 * t:(b2 + 1) * t]

    def total(a, b):
        first = jnp.logical_or(jnp.logical_not(apart), b >= a)
        second = jnp.logical_or(jnp.logical_not(apart), b < a)
        empty = jnp.zeros((t, t), F32)
        return jnp.where(first, prod[0, a, b], empty) + jnp.where(second, prod[1, a, b], empty)

    def share(k):
        for a in range(4):
            for b2 in range(2):
                give[k, a, b2] = total(a, 2 * other + b2).astype(BF)
                prod[0, a, 2 * c + b2] = total(a, 2 * c + b2)
        remote(
            give.at[k], got.at[k], pair_send.at[k], pair_recv.at[k], l, rep_of(h, y, other)
        )

    def summed(k, a, b2):
        value = prod[0, a, 2 * c + b2] + got[k, a, b2].astype(F32)
        return value

    def marked(a, b2):
        return marks_home[a, b2][0:1, :] == 1

    def owner_send(k):
        for a in range(4):
            for b2 in range(2):
                slot = mod(4 * y + 2 * c + b2 + shift - (4 * h + a) + 32, 16)
                done[k, a, b2] = jnp.where(
                    marked(a, b2), summed(k, a, b2), jnp.zeros((t, t), F32)
                ).astype(BF)
        for a in range(4):
            for b2 in range(2):
                slot = mod(4 * y + 2 * c + b2 + shift - (4 * h + a) + 32, 16)
                here, away = slot == r, slot != r

                @pl.when(here)
                def _():
                    land[k, 4 * h + a] = done[k, a, b2]

                remote(
                    done.at[k, a, b2], land.at[k, 4 * h + a], out_send.at[k, a, b2],
                    out_recv.at[k, 4 * h + a], l, slot, away,
                )

    def owner_ready(k, out_ref):
        for ap in range(8):
            jm = mod(shift + ap + r, 16)
            source = rep_of(ap // 4, div(jm, 4), div(mod(jm, 4), 2))
            arrive(land.at[k, ap], out_recv.at[k, ap], source != r)
        for ap in range(8):
            out_ref[ap, 0] = land[k, ap]

    scatter(Y)
    scatter(Z)
    home_ready(Y)
    right_start(Y)
    home_ready(Z)
    left_start(Z)
    left_forward(Z)
    right_relay(Y)
    right_start(Z)
    left_start(Y)
    for a in range(4):
        for b2 in range(2):
            arrive(marks_home.at[a, b2], mark_recv.at[a, b2], from_other(a, b2))
    left_ready(Z)
    right_ready(Y)
    multiply(Z, Y)
    share(U)
    left_forward(Y)
    right_relay(Z)
    arrive(got.at[U], pair_recv.at[U])
    rows = lax.broadcasted_iota(jnp.int32, (t, t), 0)
    cols = lax.broadcasted_iota(jnp.int32, (t, t), 1)
    for a in range(4):
        for b2 in range(2):
            on = jnp.logical_and(mod(big, 4) == y, 2 * c + b2 == a)
            eye = jnp.where(rows == cols, jnp.where(on, F32(1.5), F32(0.0)), F32(0.0))
            value = eye - 0.5 * summed(U, a, b2)
            left[U, y, a, b2] = jnp.where(marked(a, b2), value, jnp.zeros((t, t), F32)).astype(BF)
    left_start(U)
    right_start(U)
    left_forward(U)
    right_relay(U)
    right_ready(Z)
    left_ready(U)
    multiply(U, Z)
    share(Z)
    arrive(got.at[Z], pair_recv.at[Z])
    owner_send(Z)
    left_ready(Y)
    right_ready(U)
    multiply(Y, U)
    share(Y)
    arrive(got.at[Y], pair_recv.at[Y])
    owner_send(Y)
    owner_ready(Z, w_out)
    owner_ready(Y, x_out)
    for cond, copy in pending:
        if cond is None:
            copy.wait_send()
        else:
            pl.when(cond)(copy.wait_send)


def solution(mesh):
    layers = mesh.shape["layer"]

    def body(inverse_root, square_root, pattern):
        t = inverse_root.shape[-1]
        dma = pltpu.SemaphoreType.DMA
        return pl.pallas_call(
            functools.partial(kernel, layers, t),
            out_shape=[
                jax.ShapeDtypeStruct(inverse_root.shape, BF),
                jax.ShapeDtypeStruct(square_root.shape, BF),
            ],
            in_specs=[
                pl.BlockSpec(memory_space=pl.ANY),
                pl.BlockSpec(memory_space=pl.ANY),
                pl.BlockSpec(memory_space=pltpu.SMEM),
            ],
            out_specs=[pl.BlockSpec(memory_space=pltpu.VMEM)] * 2,
            scratch_shapes=[
                pltpu.VMEM((2, 8, t, t), BF),
                pltpu.VMEM((2, 8, t, t), BF),
                pltpu.VMEM((8, 8, 128), jnp.int32),
                pltpu.VMEM((4, 2, 8, 128), jnp.int32),
                pltpu.VMEM((3, 4, 4, 2, t, t), BF),
                pltpu.VMEM((3, 5, 2, 2, 2, t, t), BF),
                pltpu.VMEM((2, 4 * t, 6 * t), BF),
                pltpu.VMEM((2, 6 * t, 4 * t), BF),
                pltpu.VMEM((2, 4, 4, t, t), F32),
                pltpu.VMEM((3, 4, 2, t, t), BF),
                pltpu.VMEM((3, 4, 2, t, t), BF),
                pltpu.VMEM((2, 4, 2, t, t), BF),
                pltpu.VMEM((2, 8, t, t), BF),
                dma((2,)),
                dma((2, 8)),
                dma((2, 4, 2)),
                dma((8,)),
                dma((4, 2)),
                dma((3, 6)),
                dma((3, 6)),
                dma((3, 5, 2)),
                dma((3, 5, 2)),
                dma((3, 2)),
                dma((3,)),
                dma((3,)),
                dma((2, 4, 2)),
                dma((2, 8)),
            ],
            compiler_params=pltpu.CompilerParams(
                collective_id=0, has_side_effects=True, vmem_limit_bytes=40 * 1024 * 1024
            ),
            name="band_step",
        )(inverse_root, square_root, pattern)

    return jax.shard_map(
        body,
        mesh=mesh,
        in_specs=(P("layer", "rep", None, None), P("layer", "rep", None, None), P("layer", "rep")),
        out_specs=(P("layer", "rep", None, None), P("layer", "rep", None, None)),
        check_vma=False,
    )
```

```python
import functools

import jax
import jax.numpy as jnp
from jax import lax
from jax.experimental import pallas as pl
from jax.experimental.pallas import tpu as pltpu
from jax.sharding import PartitionSpec as P

BF = jnp.bfloat16
F32 = jnp.float32
MESH = pl.DeviceIdType.MESH
Z, Y, U = 0, 1, 2


def mod(a, b):
    return lax.rem(a, jnp.int32(b))


def div(a, b):
    return lax.div(a, jnp.int32(b))


def kernel(
    layers, t,
    z_hbm, y_hbm, pat_ref, w_out, x_out,
    raw, kept, marks, marks_home, left, right, lhs, rhs, prod, give, got, done, land,
    in_sem, home_send, home_recv, mark_send, mark_recv,
    left_send, left_recv, right_send, right_recv, pair_send, pair_recv, out_send, out_recv,
):
    l = lax.axis_index("layer")
    r = lax.axis_index("rep")
    h, y, c = div(r, 8), mod(div(r, 2), 4), mod(r, 2)
    big = 2 * l + h
    shift = 8 * mod(l + 1, 2)
    delta = mod(y + 4 * layers * 2 - big, 4)
    other = 1 - c
    pending = []

    def rep_of(hh, yy, cc):
        return hh * 8 + yy * 2 + cc

    def remote(src, dst, send_sem, recv_sem, layer, rep, cond=None):
        copy = pltpu.make_async_remote_copy(
            src_ref=src, dst_ref=dst, send_sem=send_sem, recv_sem=recv_sem,
            device_id=(layer, rep), device_id_type=MESH,
        )
        if cond is None:
            copy.start()
        else:
            pl.when(cond)(copy.start)
        pending.append((cond, copy))

    def arrive(dst, recv_sem, cond=None):
        copy = pltpu.make_async_remote_copy(
            src_ref=dst, dst_ref=dst, send_sem=recv_sem, recv_sem=recv_sem,
            device_id=(l, r), device_id_type=MESH,
        )
        if cond is None:
            copy.wait_recv()
        else:
            pl.when(cond)(copy.wait_recv)

    loads = [
        pltpu.make_async_copy(ref.at[:, 0], raw.at[k], in_sem.at[k])
        for k, ref in ((Z, z_hbm), (Y, y_hbm))
    ]
    for load in loads:
        load.start()

    barrier = pltpu.get_barrier_semaphore()
    for step in range(1, 16):
        pl.semaphore_signal(
            barrier, inc=1, device_id=(l, mod(r + step, 16)), device_id_type=MESH
        )
    above, below = l < layers - 1, l > 0
    for near, there in ((l + 1, above), (l - 1, below)):

        @pl.when(there)
        def _():
            for hh in range(2):
                for cc in range(2):
                    pl.semaphore_signal(
                        barrier, inc=1, device_id=(near, rep_of(hh, y, cc)), device_id_type=MESH
                    )


    for ap in range(8):
        marks[ap] = jnp.full((8, 128), pat_ref[ap, 0], jnp.int32)
    for k in (Z, Y):
        loads[k].wait()
        for ap in range(8):
            kept[k, ap] = jnp.where(pat_ref[ap, 0] == 1, raw[k, ap], jnp.zeros((t, t), BF))
    peers = 15 + 4 * (above.astype(jnp.int32) + below.astype(jnp.int32))
    pl.semaphore_wait(barrier, peers)

    def scatter(k):
        for ap in range(8):
            jm = mod(shift + ap + r, 16)
            yd, cd, b2 = div(jm, 4), div(mod(jm, 4), 2), mod(jm, 2)
            dest = rep_of(ap // 4, yd, cd)
            here, away = dest == r, dest != r
            a = ap % 4

            @pl.when(here)
            def _():
                left[k, yd, a, b2] = kept[k, ap]
                if k == Y:
                    marks_home[a, b2] = marks[ap]

            remote(
                kept.at[k, ap], left.at[k, yd, a, b2], home_send.at[k, ap],
                home_recv.at[k, a, b2], l, dest, away,
            )
            if k == Y:
                remote(
                    marks.at[ap], marks_home.at[a, b2], mark_send.at[ap],
                    mark_recv.at[a, b2], l, dest, away,
                )

    def from_other(a, b2):
        source = mod(4 * y + 2 * c + b2 - shift - (4 * h + a) + 32, 16)
        return source != r

    def home_ready(k):
        for a in range(4):
            for b2 in range(2):
                arrive(left.at[k, y, a, b2], home_recv.at[k, a, b2], from_other(a, b2))

    up, down = mod(y + 1, 4), mod(y + 3, 4)
    far = mod(y + 2, 4)

    def left_start(k):
        for step, half in ((0, 0), (1, 1)):
            part = pl.ds(2 * half, 2)
            remote(
                left.at[k, y, part], left.at[k, y, part], left_send.at[k, half],
                left_recv.at[k, half], l, rep_of(h, up, c),
            )
            back = 1 - half
            part = pl.ds(2 * back, 2)
            remote(
                left.at[k, y, part], left.at[k, y, part], left_send.at[k, 2 + back],
                left_recv.at[k, 2 + back], l, rep_of(h, down, c),
            )

    def left_forward(k):
        arrive(left.at[k, down, pl.ds(0, 2)], left_recv.at[k, 0])
        remote(
            left.at[k, down, pl.ds(0, 2)], left.at[k, down, pl.ds(0, 2)], left_send.at[k, 4],
            left_recv.at[k, 4], l, rep_of(h, up, c),
        )
        arrive(left.at[k, up, pl.ds(2, 2)], left_recv.at[k, 3])
        remote(
            left.at[k, up, pl.ds(2, 2)], left.at[k, up, pl.ds(2, 2)], left_send.at[k, 5],
            left_recv.at[k, 5], l, rep_of(h, down, c),
        )

    def left_ready(k):
        arrive(left.at[k, down, pl.ds(2, 2)], left_recv.at[k, 1])
        arrive(left.at[k, up, pl.ds(0, 2)], left_recv.at[k, 2])
        arrive(left.at[k, far, pl.ds(0, 2)], left_recv.at[k, 4])
        arrive(left.at[k, far, pl.ds(2, 2)], left_recv.at[k, 5])

    first, last = h == 0, h == 1
    edge_up, edge_down = mod(l, 4) == 3, mod(l, 4) == 0
    both = jnp.logical_and
    either = jnp.logical_or
    no = jnp.logical_not
    ahead = jnp.where(first, l + 1, l - 1)
    flat = no(either(both(first, edge_up), both(last, edge_down)))
    flat_behind = no(either(both(first, edge_down), both(last, edge_up)))
    cross = both(no(flat_behind), either(both(first, below), both(last, above)))

    def inside(n):
        row = big + n - 2
        return both(row >= 0, row < 2 * layers)

    def wanted(n, dl):
        return dl != (1 if n == 0 else 3)

    def chunk(k, cd, kk):
        return left.at[k, y, 2 * cd + kk]

    def right_start(k):
        def send(at, cd, kk, n, layer, rep, cond=None):
            remote(
                chunk(k, cd, kk), right.at[k, n, c, kk], right_send.at[k, at + 2 * kk + cd],
                right_recv.at[k, n, c, kk], layer, rep, cond,
            )

        for kk in (0, 1):
            for cd in range(2):
                send(0, cd, kk, 1 + 2 * h, l, rep_of(1 - h, y, cd))
        for kk in (0, 1):
            for cd in range(2):
                send(4, cd, kk, 3 - 2 * h, jnp.where(first, l - 1, l + 1), rep_of(1 - h, y, cd), cross)
        for kk in (1, 0):
            for cd in range(2):
                use = delta != 3
                inner_up = both(last, no(edge_up))
                cond = either(both(first, use), inner_up if kk == 1 else both(inner_up, use))
                send(8, cd, kk, 0, l + 1, rep_of(h, y, cd), both(above, cond))
                use = delta != 1
                inner_down = both(first, no(edge_down))
                cond = either(both(last, use), inner_down if kk == 1 else both(inner_down, use))
                send(12, cd, kk, 4, l - 1, rep_of(h, y, cd), both(below, cond))
        remote(
            left.at[k, y, pl.ds(2 * other, 2)], right.at[k, 2, c],
            right_send.at[k, 16], right_recv.at[k, 2, c, 0], l, rep_of(h, y, other),
        )
        right[k, 2, c] = left[k, y, pl.ds(2 * c, 2)]

    def right_relay(k):
        def hand(at, n_from, n_to, cc, kk, layer, rep, cond):
            remote(
                right.at[k, n_from, cc, kk], right.at[k, n_to, cc, kk], right_send.at[k, at],
                right_recv.at[k, n_to, cc, kk], layer, rep, cond,
            )

        def got_chunk(n, cc, kk, cond=None):
            arrive(right.at[k, n, cc, kk], right_recv.at[k, n, cc, kk], cond)

        def pass_on(kk):
            step = jnp.where(first, 3, 1)
            want = mod(delta + step, 4) != jnp.where(first, 1, 3)
            for cc in range(2):
                got_chunk(1 + 2 * h, cc, kk, cross)
                hand(
                    21 + 2 * kk + cc, 1 + 2 * h, 4 * h, cc, kk, l, rep_of(1 - h, y, c),
                    both(cross, want),
                )

        for cc in range(2):
            got_chunk(3 - 2 * h, cc, 0)
            hand(17 + cc, 3 - 2 * h, 1 + 2 * h, cc, 0, ahead, rep_of(h, y, c), flat)
        for cc in range(2):
            got_chunk(4 - 4 * h, cc, 1, flat)
            hand(19 + cc, 4 - 4 * h, 3 - 2 * h, cc, 1, l, rep_of(1 - h, y, c), flat)
        pass_on(0)
        pass_on(1)

    def right_ready(k):
        def got_chunk(n, cc, kk, cond=None):
            arrive(right.at[k, n, cc, kk], right_recv.at[k, n, cc, kk], cond)

        arrive(right.at[k, 2, other], right_recv.at[k, 2, other, 0])
        low = both(below, delta != 1)
        high = both(above, delta != 3)
        for cc in range(2):
            got_chunk(3 - 2 * h, cc, 1)
            for kk in range(2):
                got_chunk(1 + 2 * h, cc, kk, flat_behind)
            got_chunk(0, cc, 0, low)
            got_chunk(0, cc, 1, both(low, no(both(last, no(edge_down)))))
            got_chunk(4, cc, 0, high)
            got_chunk(4, cc, 1, both(high, no(both(first, no(edge_up)))))

    nothing = jnp.zeros((t, t), BF)
    apart = delta == 2
    toward = jnp.where(delta == 3, -1, delta)
    middle = (jnp.where(apart, -2, toward), jnp.where(apart, 2, toward))

    def multiply(kl, kr):
        for s in range(2):
            for at, n in enumerate((0, 1, 2) if s == 0 else (2, 3, 4)):
                cls = mod(big + n + 2, 4)
                gap = middle[s] - (n - 2)
                for kk in range(2):
                    inner = 2 * c + kk
                    for a in range(4):
                        tile = left[kl, cls, a, kk]
                        if n == 0:
                            tile = jnp.where(inner >= a, tile, nothing)
                        if n == 4:
                            tile = jnp.where(inner < a, tile, nothing)
                        lhs[s, a * t:(a + 1) * t, (2 * at + kk) * t:(2 * at + kk + 1) * t] = tile
                    for b in range(4):
                        whole = jnp.logical_and(gap >= -1, gap <= 1)
                        low = jnp.logical_and(gap == 2, b < inner)
                        high = jnp.logical_and(gap == -2, b >= inner)
                        good = jnp.logical_or(whole, jnp.logical_or(low, high))
                        if n != 2:
                            good = both(good, inside(n))
                        if s == 1 and n == 2:
                            good = jnp.logical_and(good, apart)
                        tile = jnp.where(good, right[kr, n, b // 2, kk, b % 2], nothing)
                        rhs[s, (2 * at + kk) * t:(2 * at + kk + 1) * t, b * t:(b + 1) * t] = tile
        for s in range(2):
            for half in range(2):
                out = jnp.dot(
                    lhs[s], rhs[s, :, half * 2 * t:(half + 1) * 2 * t], preferred_element_type=F32
                )
                for a in range(4):
                    for b2 in range(2):
                        prod[s, a, 2 * half + b2] = out[a * t:(a + 1) * t, b2 * t:(b2 + 1) * t]

    def total(a, b):
        first = jnp.logical_or(jnp.logical_not(apart), b >= a)
        second = jnp.logical_or(jnp.logical_not(apart), b < a)
        empty = jnp.zeros((t, t), F32)
        return jnp.where(first, prod[0, a, b], empty) + jnp.where(second, prod[1, a, b], empty)

    def share(k):
        for a in range(4):
            for b2 in range(2):
                give[k, a, b2] = total(a, 2 * other + b2).astype(BF)
                prod[0, a, 2 * c + b2] = total(a, 2 * c + b2)
        remote(
            give.at[k], got.at[k], pair_send.at[k], pair_recv.at[k], l, rep_of(h, y, other)
        )

    def summed(k, a, b2):
        value = prod[0, a, 2 * c + b2] + got[k, a, b2].astype(F32)
        return value

    def marked(a, b2):
        return marks_home[a, b2][0:1, :] == 1

    def owner_send(k):
        for a in range(4):
            for b2 in range(2):
                slot = mod(4 * y + 2 * c + b2 + shift - (4 * h + a) + 32, 16)
                done[k, a, b2] = jnp.where(
                    marked(a, b2), summed(k, a, b2), jnp.zeros((t, t), F32)
                ).astype(BF)
        for a in range(4):
            for b2 in range(2):
                slot = mod(4 * y + 2 * c + b2 + shift - (4 * h + a) + 32, 16)
                here, away = slot == r, slot != r

                @pl.when(here)
                def _():
                    land[k, 4 * h + a] = done[k, a, b2]

                remote(
                    done.at[k, a, b2], land.at[k, 4 * h + a], out_send.at[k, a, b2],
                    out_recv.at[k, 4 * h + a], l, slot, away,
                )

    def owner_ready(k, out_ref):
        for ap in range(8):
            jm = mod(shift + ap + r, 16)
            source = rep_of(ap // 4, div(jm, 4), div(mod(jm, 4), 2))
            arrive(land.at[k, ap], out_recv.at[k, ap], source != r)
        for ap in range(8):
            out_ref[ap, 0] = land[k, ap]

    scatter(Y)
    scatter(Z)
    home_ready(Y)
    right_start(Y)
    home_ready(Z)
    left_start(Z)
    right_relay(Y)
    left_forward(Z)
    right_start(Z)
    left_start(Y)
    for a in range(4):
        for b2 in range(2):
            arrive(marks_home.at[a, b2], mark_recv.at[a, b2], from_other(a, b2))
    left_ready(Z)
    right_ready(Y)
    multiply(Z, Y)
    share(U)
    left_forward(Y)
    right_relay(Z)
    arrive(got.at[U], pair_recv.at[U])
    rows = lax.broadcasted_iota(jnp.int32, (t, t), 0)
    cols = lax.broadcasted_iota(jnp.int32, (t, t), 1)
    for a in range(4):
        for b2 in range(2):
            on = jnp.logical_and(mod(big, 4) == y, 2 * c + b2 == a)
            eye = jnp.where(rows == cols, jnp.where(on, F32(1.5), F32(0.0)), F32(0.0))
            value = eye - 0.5 * summed(U, a, b2)
            left[U, y, a, b2] = jnp.where(marked(a, b2), value, jnp.zeros((t, t), F32)).astype(BF)
    left_start(U)
    right_start(U)
    left_forward(U)
    right_relay(U)
    right_ready(Z)
    left_ready(U)
    multiply(U, Z)
    share(Z)
    arrive(got.at[Z], pair_recv.at[Z])
    owner_send(Z)
    left_ready(Y)
    right_ready(U)
    multiply(Y, U)
    share(Y)
    arrive(got.at[Y], pair_recv.at[Y])
    owner_send(Y)
    owner_ready(Z, w_out)
    owner_ready(Y, x_out)
    for cond, copy in pending:
        if cond is None:
            copy.wait_send()
        else:
            pl.when(cond)(copy.wait_send)


def solution(mesh):
    layers = mesh.shape["layer"]

    def body(inverse_root, square_root, pattern):
        t = inverse_root.shape[-1]
        dma = pltpu.SemaphoreType.DMA
        return pl.pallas_call(
            functools.partial(kernel, layers, t),
            out_shape=[
                jax.ShapeDtypeStruct(inverse_root.shape, BF),
                jax.ShapeDtypeStruct(square_root.shape, BF),
            ],
            in_specs=[
                pl.BlockSpec(memory_space=pl.ANY),
                pl.BlockSpec(memory_space=pl.ANY),
                pl.BlockSpec(memory_space=pltpu.SMEM),
            ],
            out_specs=[pl.BlockSpec(memory_space=pltpu.VMEM)] * 2,
            scratch_shapes=[
                pltpu.VMEM((2, 8, t, t), BF),
                pltpu.VMEM((2, 8, t, t), BF),
                pltpu.VMEM((8, 8, 128), jnp.int32),
                pltpu.VMEM((4, 2, 8, 128), jnp.int32),
                pltpu.VMEM((3, 4, 4, 2, t, t), BF),
                pltpu.VMEM((3, 5, 2, 2, 2, t, t), BF),
                pltpu.VMEM((2, 4 * t, 6 * t), BF),
                pltpu.VMEM((2, 6 * t, 4 * t), BF),
                pltpu.VMEM((2, 4, 4, t, t), F32),
                pltpu.VMEM((3, 4, 2, t, t), BF),
                pltpu.VMEM((3, 4, 2, t, t), BF),
                pltpu.VMEM((2, 4, 2, t, t), BF),
                pltpu.VMEM((2, 8, t, t), BF),
                dma((2,)),
                dma((2, 8)),
                dma((2, 4, 2)),
                dma((8,)),
                dma((4, 2)),
                dma((3, 6)),
                dma((3, 6)),
                dma((3, 25)),
                dma((3, 5, 2, 2)),
                dma((3,)),
                dma((3,)),
                dma((2, 4, 2)),
                dma((2, 8)),
            ],
            compiler_params=pltpu.CompilerParams(
                collective_id=0, has_side_effects=True, vmem_limit_bytes=40 * 1024 * 1024
            ),
            name="band_step",
        )(inverse_root, square_root, pattern)

    return jax.shard_map(
        body,
        mesh=mesh,
        in_specs=(P("layer", "rep", None, None), P("layer", "rep", None, None), P("layer", "rep")),
        out_specs=(P("layer", "rep", None, None), P("layer", "rep", None, None)),
        check_vma=False,
    )
```

```python
import functools

import jax
import jax.numpy as jnp
from jax import lax
from jax.experimental import pallas as pl
from jax.experimental.pallas import tpu as pltpu
from jax.sharding import PartitionSpec as P

BF = jnp.bfloat16
F32 = jnp.float32
MESH = pl.DeviceIdType.MESH
Z, Y, U = 0, 1, 2


def mod(a, b):
    return lax.rem(a, jnp.int32(b))


def div(a, b):
    return lax.div(a, jnp.int32(b))


def kernel(
    layers, t,
    z_hbm, y_hbm, pat_ref, w_out, x_out,
    raw, kept, marks, marks_home, left, right, stage, lhs, rhs, prod, give, got, done, land,
    in_sem, home_send, home_recv, mark_send, mark_recv,
    left_send, left_recv, right_send, right_recv, stage_recv, pair_send, pair_recv, out_send, out_recv,
):
    l = lax.axis_index("layer")
    r = lax.axis_index("rep")
    h, y, c = div(r, 8), mod(div(r, 2), 4), mod(r, 2)
    big = 2 * l + h
    shift = 8 * mod(l + 1, 2)
    delta = mod(y + 4 * layers * 2 - big, 4)
    other = 1 - c
    pending = []

    def rep_of(hh, yy, cc):
        return hh * 8 + yy * 2 + cc

    def remote(src, dst, send_sem, recv_sem, layer, rep, cond=None):
        copy = pltpu.make_async_remote_copy(
            src_ref=src, dst_ref=dst, send_sem=send_sem, recv_sem=recv_sem,
            device_id=(layer, rep), device_id_type=MESH,
        )
        if cond is None:
            copy.start()
        else:
            pl.when(cond)(copy.start)
        pending.append((cond, copy))

    def arrive(dst, recv_sem, cond=None):
        copy = pltpu.make_async_remote_copy(
            src_ref=dst, dst_ref=dst, send_sem=recv_sem, recv_sem=recv_sem,
            device_id=(l, r), device_id_type=MESH,
        )
        if cond is None:
            copy.wait_recv()
        else:
            pl.when(cond)(copy.wait_recv)

    loads = [
        pltpu.make_async_copy(ref.at[:, 0], raw.at[k], in_sem.at[k])
        for k, ref in ((Z, z_hbm), (Y, y_hbm))
    ]
    for load in loads:
        load.start()

    above, below = l < layers - 1, l > 0
    first, last = h == 0, h == 1
    edge_up, edge_down = mod(l, 4) == 3, mod(l, 4) == 0
    both = jnp.logical_and
    either = jnp.logical_or
    no = jnp.logical_not
    ahead = jnp.where(first, l + 1, l - 1)
    over = 2 * h - 1
    flat = no(either(both(first, edge_up), both(last, edge_down)))
    flat_behind = no(either(both(first, edge_down), both(last, edge_up)))
    cross = both(no(flat_behind), either(both(first, below), both(last, above)))
    carry = both(no(flat), either(both(first, l >= 4), both(last, l + 4 < layers)))

    barrier = pltpu.get_barrier_semaphore()
    for step in range(1, 16):
        pl.semaphore_signal(
            barrier, inc=1, device_id=(l, mod(r + step, 16)), device_id_type=MESH
        )
    for near, there in ((l + 1, above), (l - 1, below)):

        @pl.when(there)
        def _():
            for hh in range(2):
                for cc in range(2):
                    pl.semaphore_signal(
                        barrier, inc=1, device_id=(near, rep_of(hh, y, cc)), device_id_type=MESH
                    )


    for role, hop in ((cross, -3), (carry, 3)):

        @pl.when(role)
        def _():
            for cc in range(2):
                for layer, hh in ((l + hop * over, h), (l + 4 * over, 1 - h)):
                    pl.semaphore_signal(
                        barrier, inc=1, device_id=(layer, rep_of(hh, y, cc)), device_id_type=MESH
                    )

    for ap in range(8):
        marks[ap] = jnp.full((8, 128), pat_ref[ap, 0], jnp.int32)
    for k in (Z, Y):
        loads[k].wait()
        for ap in range(8):
            kept[k, ap] = jnp.where(pat_ref[ap, 0] == 1, raw[k, ap], jnp.zeros((t, t), BF))
    peers = 15 + 4 * sum(x.astype(jnp.int32) for x in (above, below, cross, carry))
    pl.semaphore_wait(barrier, peers)

    def scatter(k):
        for ap in range(8):
            jm = mod(shift + ap + r, 16)
            yd, cd, b2 = div(jm, 4), div(mod(jm, 4), 2), mod(jm, 2)
            dest = rep_of(ap // 4, yd, cd)
            here, away = dest == r, dest != r
            a = ap % 4

            @pl.when(here)
            def _():
                left[k, yd, a, b2] = kept[k, ap]
                if k == Y:
                    marks_home[a, b2] = marks[ap]

            remote(
                kept.at[k, ap], left.at[k, yd, a, b2], home_send.at[k, ap],
                home_recv.at[k, a, b2], l, dest, away,
            )
            if k == Y:
                remote(
                    marks.at[ap], marks_home.at[a, b2], mark_send.at[ap],
                    mark_recv.at[a, b2], l, dest, away,
                )

    def from_other(a, b2):
        source = mod(4 * y + 2 * c + b2 - shift - (4 * h + a) + 32, 16)
        return source != r

    def home_ready(k):
        for a in range(4):
            for b2 in range(2):
                arrive(left.at[k, y, a, b2], home_recv.at[k, a, b2], from_other(a, b2))

    up, down = mod(y + 1, 4), mod(y + 3, 4)
    far = mod(y + 2, 4)

    def left_start(k):
        for step, half in ((0, 0), (1, 1)):
            part = pl.ds(2 * half, 2)
            remote(
                left.at[k, y, part], left.at[k, y, part], left_send.at[k, half],
                left_recv.at[k, half], l, rep_of(h, up, c),
            )
            back = 1 - half
            part = pl.ds(2 * back, 2)
            remote(
                left.at[k, y, part], left.at[k, y, part], left_send.at[k, 2 + back],
                left_recv.at[k, 2 + back], l, rep_of(h, down, c),
            )

    def left_forward(k):
        arrive(left.at[k, down, pl.ds(0, 2)], left_recv.at[k, 0])
        remote(
            left.at[k, down, pl.ds(0, 2)], left.at[k, down, pl.ds(0, 2)], left_send.at[k, 4],
            left_recv.at[k, 4], l, rep_of(h, up, c),
        )
        arrive(left.at[k, up, pl.ds(2, 2)], left_recv.at[k, 3])
        remote(
            left.at[k, up, pl.ds(2, 2)], left.at[k, up, pl.ds(2, 2)], left_send.at[k, 5],
            left_recv.at[k, 5], l, rep_of(h, down, c),
        )

    def left_ready(k):
        arrive(left.at[k, down, pl.ds(2, 2)], left_recv.at[k, 1])
        arrive(left.at[k, up, pl.ds(0, 2)], left_recv.at[k, 2])
        arrive(left.at[k, far, pl.ds(0, 2)], left_recv.at[k, 4])
        arrive(left.at[k, far, pl.ds(2, 2)], left_recv.at[k, 5])

    def inside(n):
        row = big + n - 2
        return both(row >= 0, row < 2 * layers)

    def wanted(n, dl):
        return dl != (1 if n == 0 else 3)

    def chunk(k, cd, kk):
        return left.at[k, y, 2 * cd + kk]

    def right_start(k):
        def send(at, cd, kk, n, layer, rep, cond=None):
            remote(
                chunk(k, cd, kk), right.at[k, n, c, kk], right_send.at[k, at + 2 * kk + cd],
                right_recv.at[k, n, c, kk], layer, rep, cond,
            )

        for kk in (0, 1):
            for cd in range(2):
                send(0, cd, kk, 1 + 2 * h, l, rep_of(1 - h, y, cd))
        for cd in range(2):
            send(4, cd, 0, 3 - 2 * h, l + over, rep_of(1 - h, y, cd), cross)
            remote(
                chunk(k, cd, 1), stage.at[k, 0, c], right_send.at[k, 6 + cd],
                stage_recv.at[k, 0, c], l - 3 * over, rep_of(h, y, cd), cross,
            )
            send(25, cd, 1, 4 - 4 * h, l + over, rep_of(h, y, cd), both(cross, delta != 1 + 2 * h))
        for kk in (1, 0):
            for cd in range(2):
                use = delta != 3
                cond = either(last, use) if kk == 1 else use
                send(8, cd, kk, 0, l + 1, rep_of(h, y, cd), both(no(edge_up), cond))
                use = delta != 1
                cond = either(first, use) if kk == 1 else use
                send(12, cd, kk, 4, l - 1, rep_of(h, y, cd), both(no(edge_down), cond))
        remote(
            left.at[k, y, pl.ds(2 * other, 2)], right.at[k, 2, c],
            right_send.at[k, 16], right_recv.at[k, 2, c, 0], l, rep_of(h, y, other),
        )
        right[k, 2, c] = left[k, y, pl.ds(2 * c, 2)]

    def right_relay(k):
        def hand(at, n_from, n_to, cc, kk, layer, rep, cond):
            remote(
                right.at[k, n_from, cc, kk], right.at[k, n_to, cc, kk], right_send.at[k, at],
                right_recv.at[k, n_to, cc, kk], layer, rep, cond,
            )

        def got_chunk(n, cc, kk, cond=None):
            arrive(right.at[k, n, cc, kk], right_recv.at[k, n, cc, kk], cond)

        def carried(which, kk, n, cond):
            for cc in range(2):
                arrive(stage.at[k, which, cc], stage_recv.at[k, which, cc], cond)
                remote(
                    stage.at[k, which, cc], right.at[k, n, cc, kk],
                    right_send.at[k, 33 + 2 * which + cc], right_recv.at[k, n, cc, kk],
                    l + 4 * over, rep_of(1 - h, y, c), cond,
                )

        def pass_on(kk):
            step = jnp.where(first, 3, 1)
            want = mod(delta + step, 4) != jnp.where(first, 1, 3)
            for cc in range(2):
                got_chunk(1 + 2 * h, cc, kk, cross)
                hand(
                    21 + 2 * kk + cc, 1 + 2 * h, 4 * h, cc, kk, l, rep_of(1 - h, y, c),
                    both(cross, want),
                )

        near = both(cross, delta != 2)
        for cc in range(2):
            got_chunk(3 - 2 * h, cc, 0)
            hand(17 + cc, 3 - 2 * h, 1 + 2 * h, cc, 0, ahead, rep_of(h, y, c), flat)
            remote(
                right.at[k, 3 - 2 * h, cc, 0], stage.at[k, 1, cc], right_send.at[k, 29 + cc],
                stage_recv.at[k, 1, cc], l - 3 * over, rep_of(h, y, c), near,
            )
        pass_on(0)
        carried(0, 1, 3 - 2 * h, carry)
        for cc in range(2):
            got_chunk(4 - 4 * h, cc, 1, flat)
            hand(19 + cc, 4 - 4 * h, 3 - 2 * h, cc, 1, l, rep_of(1 - h, y, c), flat)
        for cc in range(2):
            got_chunk(3 - 2 * h, cc, 1, cross)
            hand(31 + cc, 3 - 2 * h, 4 - 4 * h, cc, 1, l + over, rep_of(1 - h, y, c), near)
        carried(1, 0, 4 - 4 * h, both(carry, delta != 0))

    def right_ready(k):
        def got_chunk(n, cc, kk, cond=None):
            arrive(right.at[k, n, cc, kk], right_recv.at[k, n, cc, kk], cond)

        arrive(right.at[k, 2, other], right_recv.at[k, 2, other, 0])
        low = both(below, delta != 1)
        high = both(above, delta != 3)
        for cc in range(2):
            got_chunk(3 - 2 * h, cc, 1, no(cross))
            got_chunk(1 + 2 * h, cc, 0, flat_behind)
            got_chunk(1 + 2 * h, cc, 1, either(flat_behind, cross))
            got_chunk(0, cc, 0, low)
            got_chunk(0, cc, 1, both(low, no(both(last, no(edge_down)))))
            got_chunk(4, cc, 0, high)
            got_chunk(4, cc, 1, both(high, no(both(first, no(edge_up)))))

    nothing = jnp.zeros((t, t), BF)
    apart = delta == 2
    toward = jnp.where(delta == 3, -1, delta)
    middle = (jnp.where(apart, -2, toward), jnp.where(apart, 2, toward))

    def multiply(kl, kr):
        for s in range(2):
            for at, n in enumerate((0, 1, 2) if s == 0 else (2, 3, 4)):
                cls = mod(big + n + 2, 4)
                gap = middle[s] - (n - 2)
                for kk in range(2):
                    inner = 2 * c + kk
                    for a in range(4):
                        tile = left[kl, cls, a, kk]
                        if n == 0:
                            tile = jnp.where(inner >= a, tile, nothing)
                        if n == 4:
                            tile = jnp.where(inner < a, tile, nothing)
                        lhs[s, a * t:(a + 1) * t, (2 * at + kk) * t:(2 * at + kk + 1) * t] = tile
                    for b in range(4):
                        whole = jnp.logical_and(gap >= -1, gap <= 1)
                        low = jnp.logical_and(gap == 2, b < inner)
                        high = jnp.logical_and(gap == -2, b >= inner)
                        good = jnp.logical_or(whole, jnp.logical_or(low, high))
                        if n != 2:
                            good = both(good, inside(n))
                        if s == 1 and n == 2:
                            good = jnp.logical_and(good, apart)
                        tile = jnp.where(good, right[kr, n, b // 2, kk, b % 2], nothing)
                        rhs[s, (2 * at + kk) * t:(2 * at + kk + 1) * t, b * t:(b + 1) * t] = tile
        for s in range(2):
            for half in range(2):
                out = jnp.dot(
                    lhs[s], rhs[s, :, half * 2 * t:(half + 1) * 2 * t], preferred_element_type=F32
                )
                for a in range(4):
                    for b2 in range(2):
                        prod[s, a, 2 * half + b2] = out[a * t:(a + 1) * t, b2 * t:(b2 + 1) * t]

    def total(a, b):
        first = jnp.logical_or(jnp.logical_not(apart), b >= a)
        second = jnp.logical_or(jnp.logical_not(apart), b < a)
        empty = jnp.zeros((t, t), F32)
        return jnp.where(first, prod[0, a, b], empty) + jnp.where(second, prod[1, a, b], empty)

    def share(k):
        for a in range(4):
            for b2 in range(2):
                give[k, a, b2] = total(a, 2 * other + b2).astype(BF)
                prod[0, a, 2 * c + b2] = total(a, 2 * c + b2)
        remote(
            give.at[k], got.at[k], pair_send.at[k], pair_recv.at[k], l, rep_of(h, y, other)
        )

    def summed(k, a, b2):
        value = prod[0, a, 2 * c + b2] + got[k, a, b2].astype(F32)
        return value

    def marked(a, b2):
        return marks_home[a, b2][0:1, :] == 1

    def owner_send(k):
        for a in range(4):
            for b2 in range(2):
                slot = mod(4 * y + 2 * c + b2 + shift - (4 * h + a) + 32, 16)
                done[k, a, b2] = jnp.where(
                    marked(a, b2), summed(k, a, b2), jnp.zeros((t, t), F32)
                ).astype(BF)
        for a in range(4):
            for b2 in range(2):
                slot = mod(4 * y + 2 * c + b2 + shift - (4 * h + a) + 32, 16)
                here, away = slot == r, slot != r

                @pl.when(here)
                def _():
                    land[k, 4 * h + a] = done[k, a, b2]

                remote(
                    done.at[k, a, b2], land.at[k, 4 * h + a], out_send.at[k, a, b2],
                    out_recv.at[k, 4 * h + a], l, slot, away,
                )

    def owner_ready(k, out_ref):
        for ap in range(8):
            jm = mod(shift + ap + r, 16)
            source = rep_of(ap // 4, div(jm, 4), div(mod(jm, 4), 2))
            arrive(land.at[k, ap], out_recv.at[k, ap], source != r)
        for ap in range(8):
            out_ref[ap, 0] = land[k, ap]

    scatter(Y)
    scatter(Z)
    home_ready(Y)
    right_start(Y)
    home_ready(Z)
    left_start(Z)
    right_relay(Y)
    left_forward(Z)
    right_start(Z)
    left_start(Y)
    for a in range(4):
        for b2 in range(2):
            arrive(marks_home.at[a, b2], mark_recv.at[a, b2], from_other(a, b2))
    left_ready(Z)
    right_ready(Y)
    multiply(Z, Y)
    share(U)
    left_forward(Y)
    right_relay(Z)
    arrive(got.at[U], pair_recv.at[U])
    rows = lax.broadcasted_iota(jnp.int32, (t, t), 0)
    cols = lax.broadcasted_iota(jnp.int32, (t, t), 1)
    for a in range(4):
        for b2 in range(2):
            on = jnp.logical_and(mod(big, 4) == y, 2 * c + b2 == a)
            eye = jnp.where(rows == cols, jnp.where(on, F32(1.5), F32(0.0)), F32(0.0))
            value = eye - 0.5 * summed(U, a, b2)
            left[U, y, a, b2] = jnp.where(marked(a, b2), value, jnp.zeros((t, t), F32)).astype(BF)
    left_start(U)
    right_start(U)
    left_forward(U)
    right_relay(U)
    right_ready(Z)
    left_ready(U)
    multiply(U, Z)
    share(Z)
    arrive(got.at[Z], pair_recv.at[Z])
    owner_send(Z)
    left_ready(Y)
    right_ready(U)
    multiply(Y, U)
    share(Y)
    arrive(got.at[Y], pair_recv.at[Y])
    owner_send(Y)
    owner_ready(Z, w_out)
    owner_ready(Y, x_out)
    for cond, copy in pending:
        if cond is None:
            copy.wait_send()
        else:
            pl.when(cond)(copy.wait_send)


def solution(mesh):
    layers = mesh.shape["layer"]

    def body(inverse_root, square_root, pattern):
        t = inverse_root.shape[-1]
        dma = pltpu.SemaphoreType.DMA
        return pl.pallas_call(
            functools.partial(kernel, layers, t),
            out_shape=[
                jax.ShapeDtypeStruct(inverse_root.shape, BF),
                jax.ShapeDtypeStruct(square_root.shape, BF),
            ],
            in_specs=[
                pl.BlockSpec(memory_space=pl.ANY),
                pl.BlockSpec(memory_space=pl.ANY),
                pl.BlockSpec(memory_space=pltpu.SMEM),
            ],
            out_specs=[pl.BlockSpec(memory_space=pltpu.VMEM)] * 2,
            scratch_shapes=[
                pltpu.VMEM((2, 8, t, t), BF),
                pltpu.VMEM((2, 8, t, t), BF),
                pltpu.VMEM((8, 8, 128), jnp.int32),
                pltpu.VMEM((4, 2, 8, 128), jnp.int32),
                pltpu.VMEM((3, 4, 4, 2, t, t), BF),
                pltpu.VMEM((3, 5, 2, 2, 2, t, t), BF),
                pltpu.VMEM((3, 2, 2, 2, t, t), BF),
                pltpu.VMEM((2, 4 * t, 6 * t), BF),
                pltpu.VMEM((2, 6 * t, 4 * t), BF),
                pltpu.VMEM((2, 4, 4, t, t), F32),
                pltpu.VMEM((3, 4, 2, t, t), BF),
                pltpu.VMEM((3, 4, 2, t, t), BF),
                pltpu.VMEM((2, 4, 2, t, t), BF),
                pltpu.VMEM((2, 8, t, t), BF),
                dma((2,)),
                dma((2, 8)),
                dma((2, 4, 2)),
                dma((8,)),
                dma((4, 2)),
                dma((3, 6)),
                dma((3, 6)),
                dma((3, 37)),
                dma((3, 5, 2, 2)),
                dma((3, 2, 2)),
                dma((3,)),
                dma((3,)),
                dma((2, 4, 2)),
                dma((2, 8)),
            ],
            compiler_params=pltpu.CompilerParams(
                collective_id=0, has_side_effects=True, vmem_limit_bytes=40 * 1024 * 1024
            ),
            name="band_step",
        )(inverse_root, square_root, pattern)

    return jax.shard_map(
        body,
        mesh=mesh,
        in_specs=(P("layer", "rep", None, None), P("layer", "rep", None, None), P("layer", "rep")),
        out_specs=(P("layer", "rep", None, None), P("layer", "rep", None, None)),
        check_vma=False,
    )
```

```python
import functools

import jax
import jax.numpy as jnp
from jax import lax
from jax.experimental import pallas as pl
from jax.experimental.pallas import tpu as pltpu
from jax.sharding import PartitionSpec as P

BF = jnp.bfloat16
F32 = jnp.float32
MESH = pl.DeviceIdType.MESH
Z, Y, U = 0, 1, 2


def mod(a, b):
    return lax.rem(a, jnp.int32(b))


def div(a, b):
    return lax.div(a, jnp.int32(b))


def kernel(
    layers, t,
    z_hbm, y_hbm, pat_ref, w_out, x_out,
    raw, kept, marks, marks_home, left, right, stage, lhs, rhs, prod, give, got, done,
    in_sem, home_send, home_recv, mark_send, mark_recv,
    left_send, left_recv, right_send, right_recv, stage_recv, pair_send, pair_recv, out_send, out_recv, self_sem,
):
    l = lax.axis_index("layer")
    r = lax.axis_index("rep")
    h, y, c = div(r, 8), mod(div(r, 2), 4), mod(r, 2)
    big = 2 * l + h
    shift = 8 * mod(l + 1, 2)
    delta = mod(y + 4 * layers * 2 - big, 4)
    other = 1 - c
    pending = []
    kept_here = []

    def rep_of(hh, yy, cc):
        return hh * 8 + yy * 2 + cc

    def remote(src, dst, send_sem, recv_sem, layer, rep, cond=None):
        copy = pltpu.make_async_remote_copy(
            src_ref=src, dst_ref=dst, send_sem=send_sem, recv_sem=recv_sem,
            device_id=(layer, rep), device_id_type=MESH,
        )
        if cond is None:
            copy.start()
        else:
            pl.when(cond)(copy.start)
        pending.append((cond, copy))

    def arrive(dst, recv_sem, cond=None):
        copy = pltpu.make_async_remote_copy(
            src_ref=dst, dst_ref=dst, send_sem=recv_sem, recv_sem=recv_sem,
            device_id=(l, r), device_id_type=MESH,
        )
        if cond is None:
            copy.wait_recv()
        else:
            pl.when(cond)(copy.wait_recv)

    loads = [
        pltpu.make_async_copy(ref.at[:, 0], raw.at[k], in_sem.at[k])
        for k, ref in ((Z, z_hbm), (Y, y_hbm))
    ]
    for load in loads:
        load.start()

    above, below = l < layers - 1, l > 0
    first, last = h == 0, h == 1
    edge_up, edge_down = mod(l, 4) == 3, mod(l, 4) == 0
    both = jnp.logical_and
    either = jnp.logical_or
    no = jnp.logical_not
    ahead = jnp.where(first, l + 1, l - 1)
    over = 2 * h - 1
    flat = no(either(both(first, edge_up), both(last, edge_down)))
    flat_behind = no(either(both(first, edge_down), both(last, edge_up)))
    cross = both(no(flat_behind), either(both(first, below), both(last, above)))
    carry = both(no(flat), either(both(first, l >= 4), both(last, l + 4 < layers)))

    barrier = pltpu.get_barrier_semaphore()
    for step in range(1, 16):
        pl.semaphore_signal(
            barrier, inc=1, device_id=(l, mod(r + step, 16)), device_id_type=MESH
        )
    for near, there in ((l + 1, above), (l - 1, below)):

        @pl.when(there)
        def _():
            for hh in range(2):
                for cc in range(2):
                    pl.semaphore_signal(
                        barrier, inc=1, device_id=(near, rep_of(hh, y, cc)), device_id_type=MESH
                    )


    for role, hop in ((cross, -3), (carry, 3)):

        @pl.when(role)
        def _():
            for cc in range(2):
                for layer, hh in ((l + hop * over, h), (l + 4 * over, 1 - h)):
                    pl.semaphore_signal(
                        barrier, inc=1, device_id=(layer, rep_of(hh, y, cc)), device_id_type=MESH
                    )

    for ap in range(8):
        marks[ap] = jnp.full((8, 128), pat_ref[ap], jnp.int32)
    for k in (Z, Y):
        loads[k].wait()
        for ap in range(8):
            kept[k, ap] = jnp.where(pat_ref[ap] == 1, raw[k, ap], jnp.zeros((t, t), BF))
    peers = 15 + 4 * sum(x.astype(jnp.int32) for x in (above, below, cross, carry))
    pl.semaphore_wait(barrier, peers)

    def scatter(k):
        for ap in (0, 4, 2, 6, 1, 5, 3, 7):
            jm = mod(shift + ap + r, 16)
            yd, cd, b2 = div(jm, 4), div(mod(jm, 4), 2), mod(jm, 2)
            dest = rep_of(ap // 4, yd, cd)
            here, away = dest == r, dest != r
            a = ap % 4

            @pl.when(here)
            def _():
                left[k, yd, a, b2] = kept[k, ap]
                if k == Y:
                    marks_home[a, b2] = marks[ap]

            remote(
                kept.at[k, ap], left.at[k, yd, a, b2], home_send.at[k, ap],
                home_recv.at[k, a, b2], l, dest, away,
            )
            if k == Y:
                remote(
                    marks.at[ap], marks_home.at[a, b2], mark_send.at[ap],
                    mark_recv.at[a, b2], l, dest, away,
                )

    def from_other(a, b2):
        source = mod(4 * y + 2 * c + b2 - shift - (4 * h + a) + 32, 16)
        return source != r

    def home_ready(k, rows=(0, 1, 2, 3)):
        for a in rows:
            for b2 in range(2):
                arrive(left.at[k, y, a, b2], home_recv.at[k, a, b2], from_other(a, b2))

    up, down = mod(y + 1, 4), mod(y + 3, 4)
    far = mod(y + 2, 4)

    def left_start(k):
        for step, half in ((0, 0), (1, 1)):
            part = pl.ds(2 * half, 2)
            remote(
                left.at[k, y, part], left.at[k, y, part], left_send.at[k, half],
                left_recv.at[k, half], l, rep_of(h, up, c),
            )
            back = 1 - half
            part = pl.ds(2 * back, 2)
            remote(
                left.at[k, y, part], left.at[k, y, part], left_send.at[k, 2 + back],
                left_recv.at[k, 2 + back], l, rep_of(h, down, c),
            )

    def left_forward(k):
        arrive(left.at[k, down, pl.ds(0, 2)], left_recv.at[k, 0])
        remote(
            left.at[k, down, pl.ds(0, 2)], left.at[k, down, pl.ds(0, 2)], left_send.at[k, 4],
            left_recv.at[k, 4], l, rep_of(h, up, c),
        )
        arrive(left.at[k, up, pl.ds(2, 2)], left_recv.at[k, 3])
        remote(
            left.at[k, up, pl.ds(2, 2)], left.at[k, up, pl.ds(2, 2)], left_send.at[k, 5],
            left_recv.at[k, 5], l, rep_of(h, down, c),
        )

    def left_ready(k):
        arrive(left.at[k, down, pl.ds(2, 2)], left_recv.at[k, 1])
        arrive(left.at[k, up, pl.ds(0, 2)], left_recv.at[k, 2])
        arrive(left.at[k, far, pl.ds(0, 2)], left_recv.at[k, 4])
        arrive(left.at[k, far, pl.ds(2, 2)], left_recv.at[k, 5])

    def inside(n):
        row = big + n - 2
        return both(row >= 0, row < 2 * layers)

    def wanted(n, dl):
        return dl != (1 if n == 0 else 3)

    def chunk(k, cd, kk):
        return left.at[k, y, 2 * cd + kk]

    def right_start(k, rows_of=None):
        def home(*rows):
            if rows_of is not None:
                rows_of(k, rows)

        def send(at, cd, kk, n, layer, rep, cond=None):
            remote(
                chunk(k, cd, kk), right.at[k, n, c, kk], right_send.at[k, at + 2 * kk + cd],
                right_recv.at[k, n, c, kk], layer, rep, cond,
            )

        for cd in range(2):
            home(2 * cd)
            send(0, cd, 0, 1 + 2 * h, l, rep_of(1 - h, y, cd))
        home(1, 3)
        for cd in range(2):
            send(0, cd, 1, 1 + 2 * h, l, rep_of(1 - h, y, cd))
        for cd in range(2):
            send(4, cd, 0, 3 - 2 * h, l + over, rep_of(1 - h, y, cd), cross)
            remote(
                chunk(k, cd, 1), stage.at[k, 0, c], right_send.at[k, 6 + cd],
                stage_recv.at[k, 0, c], l - 3 * over, rep_of(h, y, cd), cross,
            )
            send(25, cd, 1, 4 - 4 * h, l + over, rep_of(h, y, cd), both(cross, delta != 1 + 2 * h))
        for kk in (1, 0):
            for cd in range(2):
                use = delta != 3
                cond = either(last, use) if kk == 1 else use
                send(8, cd, kk, 0, l + 1, rep_of(h, y, cd), both(no(edge_up), cond))
                use = delta != 1
                cond = either(first, use) if kk == 1 else use
                send(12, cd, kk, 4, l - 1, rep_of(h, y, cd), both(no(edge_down), cond))
        remote(
            left.at[k, y, pl.ds(2 * other, 2)], right.at[k, 2, c],
            right_send.at[k, 16], right_recv.at[k, 2, c, 0], l, rep_of(h, y, other),
        )
        right[k, 2, c] = left[k, y, pl.ds(2 * c, 2)]

    def right_relay(k, parts=(0, 1, 2)):
        def hand(at, n_from, n_to, cc, kk, layer, rep, cond):
            remote(
                right.at[k, n_from, cc, kk], right.at[k, n_to, cc, kk], right_send.at[k, at],
                right_recv.at[k, n_to, cc, kk], layer, rep, cond,
            )

        def got_chunk(n, cc, kk, cond=None):
            arrive(right.at[k, n, cc, kk], right_recv.at[k, n, cc, kk], cond)

        def carried(which, kk, n, cond):
            for cc in range(2):
                arrive(stage.at[k, which, cc], stage_recv.at[k, which, cc], cond)
                remote(
                    stage.at[k, which, cc], right.at[k, n, cc, kk],
                    right_send.at[k, 33 + 2 * which + cc], right_recv.at[k, n, cc, kk],
                    l + 4 * over, rep_of(1 - h, y, c), cond,
                )

        def pass_on(kk):
            step = jnp.where(first, 3, 1)
            want = mod(delta + step, 4) != jnp.where(first, 1, 3)
            for cc in range(2):
                got_chunk(1 + 2 * h, cc, kk, cross)
                hand(
                    21 + 2 * kk + cc, 1 + 2 * h, 4 * h, cc, kk, l, rep_of(1 - h, y, c),
                    both(cross, want),
                )

        near = both(cross, delta != 2)
        if 0 in parts:
            for cc in range(2):
                got_chunk(3 - 2 * h, cc, 0)
                hand(17 + cc, 3 - 2 * h, 1 + 2 * h, cc, 0, ahead, rep_of(h, y, c), flat)
                hand(29 + cc, 3 - 2 * h, 4 - 4 * h, cc, 0, l + over, rep_of(1 - h, y, c), near)
            pass_on(0)
        if 1 in parts:
            carried(0, 1, 3 - 2 * h, carry)
            for cc in range(2):
                got_chunk(4 - 4 * h, cc, 1, flat)
                hand(19 + cc, 4 - 4 * h, 3 - 2 * h, cc, 1, l, rep_of(1 - h, y, c), flat)
        if 2 in parts:
            for cc in range(2):
                got_chunk(3 - 2 * h, cc, 1, cross)
                hand(31 + cc, 3 - 2 * h, 4 - 4 * h, cc, 1, l + over, rep_of(1 - h, y, c), near)

    def right_ready(k):
        def got_chunk(n, cc, kk, cond=None):
            arrive(right.at[k, n, cc, kk], right_recv.at[k, n, cc, kk], cond)

        arrive(right.at[k, 2, other], right_recv.at[k, 2, other, 0])
        low = both(below, delta != 1)
        high = both(above, delta != 3)
        for cc in range(2):
            got_chunk(3 - 2 * h, cc, 1, no(cross))
            got_chunk(1 + 2 * h, cc, 0, flat_behind)
            got_chunk(1 + 2 * h, cc, 1, either(flat_behind, cross))
            got_chunk(0, cc, 0, low)
            got_chunk(0, cc, 1, both(low, no(both(last, no(edge_down)))))
            got_chunk(4, cc, 0, high)
            got_chunk(4, cc, 1, both(high, no(both(first, no(edge_up)))))

    nothing = jnp.zeros((t, t), BF)
    apart = delta == 2
    toward = jnp.where(delta == 3, -1, delta)
    middle = (jnp.where(apart, -2, toward), jnp.where(apart, 2, toward))

    def build_left(kl):
        for s in range(2):
            for at, n in enumerate((0, 1, 2) if s == 0 else (2, 3, 4)):
                cls = mod(big + n + 2, 4)
                for kk in range(2):
                    inner = 2 * c + kk
                    for a in range(4):
                        tile = left[kl, cls, a, kk]
                        if n == 0:
                            tile = jnp.where(inner >= a, tile, nothing)
                        if n == 4:
                            tile = jnp.where(inner < a, tile, nothing)
                        lhs[s, a * t:(a + 1) * t, (2 * at + kk) * t:(2 * at + kk + 1) * t] = tile

    def build_right(kr, rows):
        for s in range(2):
            for at, n in enumerate((0, 1, 2) if s == 0 else (2, 3, 4)):
                if n not in rows:
                    continue
                gap = middle[s] - (n - 2)
                for kk in range(2):
                    inner = 2 * c + kk
                    for b in range(4):
                        whole = jnp.logical_and(gap >= -1, gap <= 1)
                        low = jnp.logical_and(gap == 2, b < inner)
                        high = jnp.logical_and(gap == -2, b >= inner)
                        good = jnp.logical_or(whole, jnp.logical_or(low, high))
                        if n != 2:
                            good = both(good, inside(n))
                        if s == 1 and n == 2:
                            good = jnp.logical_and(good, apart)
                        tile = jnp.where(good, right[kr, n, b // 2, kk, b % 2], nothing)
                        rhs[s, b // 2, (2 * at + kk) * t:(2 * at + kk + 1) * t, (b % 2) * t:(b % 2 + 1) * t] = tile

    def columns(half):
        first_out = jnp.dot(lhs[0], rhs[0, half], preferred_element_type=F32)
        second_out = jnp.dot(lhs[1], rhs[1, half], preferred_element_type=F32)

        def value(a, b2):
            b = 2 * half + b2
            use_first = either(no(apart), b >= a)
            use_second = either(no(apart), b < a)
            empty = jnp.zeros((t, t), F32)
            x = first_out[a * t:(a + 1) * t, b2 * t:(b2 + 1) * t]
            z = second_out[a * t:(a + 1) * t, b2 * t:(b2 + 1) * t]
            return jnp.where(use_first, x, empty) + jnp.where(use_second, z, empty)

        return value

    def multiply(k):
        part = columns(other)
        for a in range(4):
            for b2 in range(2):
                give[k, a, b2] = part(a, b2).astype(BF)
        remote(
            give.at[k], got.at[k], pair_send.at[k], pair_recv.at[k], l, rep_of(h, y, other)
        )
        part = columns(c)
        for a in range(4):
            for b2 in range(2):
                prod[a, b2] = part(a, b2)

    def summed(k, a, b2):
        value = prod[a, b2] + got[k, a, b2].astype(F32)
        return value

    def marked(a, b2):
        return marks_home[a, b2][0:1, :] == 1

    def owner_send(k, out_ref):
        for a in range(4):
            for b2 in range(2):
                done[k, a, b2] = jnp.where(
                    marked(a, b2), summed(k, a, b2), jnp.zeros((t, t), F32)
                ).astype(BF)
        for a in range(4):
            for b2 in range(2):
                slot = mod(4 * y + 2 * c + b2 + shift - (4 * h + a) + 32, 16)
                here = slot == r
                mine = pltpu.make_async_copy(
                    done.at[k, a, b2], out_ref.at[4 * h + a, 0], self_sem.at[k, a, b2]
                )
                pl.when(here)(mine.start)
                kept_here.append((here, mine))
                remote(
                    done.at[k, a, b2], out_ref.at[4 * h + a, 0], out_send.at[k, a, b2],
                    out_recv.at[k, 4 * h + a], l, slot, slot != r,
                )

    def owner_ready(k, out_ref):
        for ap in range(8):
            jm = mod(shift + ap + r, 16)
            source = rep_of(ap // 4, div(jm, 4), div(mod(jm, 4), 2))
            arrive(out_ref.at[ap, 0], out_recv.at[k, ap], source != r)

    def marks_ready():
        for a in range(4):
            for b2 in range(2):
                arrive(marks_home.at[a, b2], mark_recv.at[a, b2], from_other(a, b2))

    def finish_u():
        arrive(got.at[U], pair_recv.at[U])
        rows = lax.broadcasted_iota(jnp.int32, (t, t), 0)
        cols = lax.broadcasted_iota(jnp.int32, (t, t), 1)
        for a in range(4):
            for b2 in range(2):
                on = jnp.logical_and(mod(big, 4) == y, 2 * c + b2 == a)
                eye = jnp.where(rows == cols, jnp.where(on, F32(1.5), F32(0.0)), F32(0.0))
                value = eye - 0.5 * summed(U, a, b2)
                left[U, y, a, b2] = jnp.where(marked(a, b2), value, jnp.zeros((t, t), F32)).astype(BF)

    scatter(Y)
    scatter(Z)
    right_start(Y, home_ready)
    home_ready(Z)
    left_start(Z)
    right_relay(Y, (0,))
    left_forward(Z)
    right_relay(Y, (1, 2))
    right_start(Z)
    left_start(Y)
    marks_ready()
    left_ready(Z)
    build_left(Z)
    right_ready(Y)
    build_right(Y, (0, 1, 2, 3, 4))
    multiply(U)
    left_forward(Y)
    right_relay(Z)
    finish_u()
    left_start(U)
    right_start(U)
    left_forward(U)
    right_relay(U)
    right_ready(Z)
    build_right(Z, (0, 1, 2, 3, 4))
    left_ready(U)
    build_left(U)
    multiply(Z)
    arrive(got.at[Z], pair_recv.at[Z])
    owner_send(Z, w_out)
    left_ready(Y)
    build_left(Y)
    right_ready(U)
    build_right(U, (0, 1, 2, 3, 4))
    multiply(Y)
    arrive(got.at[Y], pair_recv.at[Y])
    owner_send(Y, x_out)
    owner_ready(Z, w_out)
    owner_ready(Y, x_out)
    for cond, copy in kept_here:
        pl.when(cond)(copy.wait)
    for cond, copy in pending:
        if cond is None:
            copy.wait_send()
        else:
            pl.when(cond)(copy.wait_send)


def solution(mesh):
    layers = mesh.shape["layer"]

    def body(inverse_root, square_root, pattern):
        t = inverse_root.shape[-1]
        dma = pltpu.SemaphoreType.DMA
        return pl.pallas_call(
            functools.partial(kernel, layers, t),
            out_shape=[
                jax.ShapeDtypeStruct(inverse_root.shape, BF),
                jax.ShapeDtypeStruct(square_root.shape, BF),
            ],
            in_specs=[
                pl.BlockSpec(memory_space=pl.ANY),
                pl.BlockSpec(memory_space=pl.ANY),
                pl.BlockSpec(memory_space=pltpu.SMEM),
            ],
            out_specs=[pl.BlockSpec(memory_space=pl.ANY)] * 2,
            scratch_shapes=[
                pltpu.VMEM((2, 8, t, t), BF),
                pltpu.VMEM((2, 8, t, t), BF),
                pltpu.VMEM((8, 8, 128), jnp.int32),
                pltpu.VMEM((4, 2, 8, 128), jnp.int32),
                pltpu.VMEM((3, 4, 4, 2, t, t), BF),
                pltpu.VMEM((3, 5, 2, 2, 2, t, t), BF),
                pltpu.VMEM((3, 2, 2, 2, t, t), BF),
                pltpu.VMEM((2, 4 * t, 6 * t), BF),
                pltpu.VMEM((2, 2, 6 * t, 2 * t), BF),
                pltpu.VMEM((4, 2, t, t), F32),
                pltpu.VMEM((3, 4, 2, t, t), BF),
                pltpu.VMEM((3, 4, 2, t, t), BF),
                pltpu.VMEM((2, 4, 2, t, t), BF),
                dma((2,)),
                dma((2, 8)),
                dma((2, 4, 2)),
                dma((8,)),
                dma((4, 2)),
                dma((3, 6)),
                dma((3, 6)),
                dma((3, 37)),
                dma((3, 5, 2, 2)),
                dma((3, 2, 2)),
                dma((3,)),
                dma((3,)),
                dma((2, 4, 2)),
                dma((2, 8)),
                dma((2, 4, 2)),
            ],
            compiler_params=pltpu.CompilerParams(
                collective_id=0, has_side_effects=True, vmem_limit_bytes=67043328
            ),
            name="band_step",
        )(inverse_root, square_root, pattern.reshape(-1))

    return jax.shard_map(
        body,
        mesh=mesh,
        in_specs=(P("layer", "rep", None, None), P("layer", "rep", None, None), P("layer", "rep")),
        out_specs=(P("layer", "rep", None, None), P("layer", "rep", None, None)),
        check_vma=False,
    )
```

```python
import functools

import jax
import jax.numpy as jnp
from jax import lax
from jax.experimental import pallas as pl
from jax.experimental.pallas import tpu as pltpu
from jax.sharding import PartitionSpec as P

BF = jnp.bfloat16
F32 = jnp.float32
MESH = pl.DeviceIdType.MESH
Z, Y, U = 0, 1, 2


def mod(a, b):
    return lax.rem(a, jnp.int32(b))


def div(a, b):
    return lax.div(a, jnp.int32(b))


def kernel(
    layers, t,
    z_hbm, y_hbm, pat_hbm, w_out, x_out,
    pat_ref, raw, kept, marks, marks_home, left, right, stage, lhs, rhs, prod, give, got, done,
    in_sem, home_send, home_recv, mark_send, mark_recv,
    left_send, left_recv, right_send, right_recv, stage_recv, pair_send, pair_recv, out_send, out_recv, self_sem,
):
    l = lax.axis_index("layer")
    r = lax.axis_index("rep")
    h, y, c = div(r, 8), mod(div(r, 2), 4), mod(r, 2)
    big = 2 * l + h
    shift = 8 * mod(l + 1, 2)
    delta = mod(y + 4 * layers * 2 - big, 4)
    other = 1 - c
    pending = []
    kept_here = []

    def rep_of(hh, yy, cc):
        return hh * 8 + yy * 2 + cc

    def remote(src, dst, send_sem, recv_sem, layer, rep, cond=None):
        copy = pltpu.make_async_remote_copy(
            src_ref=src, dst_ref=dst, send_sem=send_sem, recv_sem=recv_sem,
            device_id=(layer, rep), device_id_type=MESH,
        )
        if cond is None:
            copy.start()
        else:
            pl.when(cond)(copy.start)

    def settle(size, send_sem, cond=None):
        copy = pltpu.make_async_remote_copy(
            src_ref=size, dst_ref=size, send_sem=send_sem, recv_sem=send_sem,
            device_id=(l, r), device_id_type=MESH,
        )
        pending.append((cond, copy))

    def arrive(dst, recv_sem, cond=None):
        copy = pltpu.make_async_remote_copy(
            src_ref=dst, dst_ref=dst, send_sem=recv_sem, recv_sem=recv_sem,
            device_id=(l, r), device_id_type=MESH,
        )
        if cond is None:
            copy.wait_recv()
        else:
            pl.when(cond)(copy.wait_recv)

    loads = [
        pltpu.make_async_copy(ref.at[:, 0], raw.at[k], in_sem.at[k])
        for k, ref in ((Z, z_hbm), (Y, y_hbm))
    ]
    pat_load = pltpu.make_async_copy(pat_hbm, pat_ref, in_sem.at[2])
    pat_load.start()
    for load in loads:
        load.start()

    above, below = l < layers - 1, l > 0
    first, last = h == 0, h == 1
    edge_up, edge_down = mod(l, 4) == 3, mod(l, 4) == 0
    both = jnp.logical_and
    either = jnp.logical_or
    no = jnp.logical_not
    ahead = jnp.where(first, l + 1, l - 1)
    over = 2 * h - 1
    flat = no(either(both(first, edge_up), both(last, edge_down)))
    flat_behind = no(either(both(first, edge_down), both(last, edge_up)))
    cross = both(no(flat_behind), either(both(first, below), both(last, above)))
    carry = both(no(flat), either(both(first, l >= 4), both(last, l + 4 < layers)))

    barrier = pltpu.get_barrier_semaphore()
    for step in range(1, 16):
        pl.semaphore_signal(
            barrier, inc=1, device_id=(l, mod(r + step, 16)), device_id_type=MESH
        )
    for near, there in ((l + 1, above), (l - 1, below)):

        @pl.when(there)
        def _():
            for hh in range(2):
                for cc in range(2):
                    pl.semaphore_signal(
                        barrier, inc=1, device_id=(near, rep_of(hh, y, cc)), device_id_type=MESH
                    )


    for role, hop in ((cross, -3), (carry, 3)):

        @pl.when(role)
        def _():
            for cc in range(2):
                for layer, hh in ((l + hop * over, h), (l + 4 * over, 1 - h)):
                    pl.semaphore_signal(
                        barrier, inc=1, device_id=(layer, rep_of(hh, y, cc)), device_id_type=MESH
                    )

    pat_load.wait()
    for ap in range(8):
        marks[ap] = jnp.full((8, 128), pat_ref[ap], jnp.int32)
    for k in (Z, Y):
        loads[k].wait()
        for ap in range(8):
            kept[k, ap] = jnp.where(pat_ref[ap] == 1, raw[k, ap], jnp.zeros((t, t), BF))
    peers = 15 + 4 * sum(x.astype(jnp.int32) for x in (above, below, cross, carry))
    pl.semaphore_wait(barrier, peers)

    def home_of(ap):
        jm = mod(shift + ap + r, 16)
        return div(jm, 4), div(mod(jm, 4), 2), mod(jm, 2)

    def to_rep(ap):
        yd, cd, _ = home_of(ap)
        return rep_of(ap // 4, yd, cd)

    staying = sum((to_rep(ap) == r).astype(jnp.int32) for ap in range(8))

    def moved(ref, sem):
        for n in (6, 7, 8):
            settle(ref.at[pl.ds(0, n)], sem, 8 - staying == n)

    def arrived(ref, sem):
        for n in (6, 7, 8):
            arrive(ref.at[pl.ds(0, n)], sem, 8 - staying == n)

    def scatter(k):
        for ap in (0, 4, 2, 6, 1, 5, 3, 7):
            yd, cd, b2 = home_of(ap)
            dest = rep_of(ap // 4, yd, cd)
            here, away = dest == r, dest != r
            a = ap % 4

            @pl.when(here)
            def _():
                left[k, yd, a, b2] = kept[k, ap]
                if k == Y:
                    marks_home[a, b2] = marks[ap]

            remote(
                kept.at[k, ap], left.at[k, yd, a, b2], home_send.at[k], home_recv.at[k],
                l, dest, away,
            )
            if k == Y:
                remote(
                    marks.at[ap], marks_home.at[a, b2], mark_send, mark_recv, l, dest, away
                )
        moved(kept.at[k], home_send.at[k])
        if k == Y:
            moved(marks, mark_send)

    def home_ready(k):
        arrived(kept.at[k], home_recv.at[k])

    up, down = mod(y + 1, 4), mod(y + 3, 4)
    far = mod(y + 2, 4)

    def half_of(k, whose, half):
        return left.at[k, whose, pl.ds(2 * half, 2)]

    def left_send_half(k, whose, half, at, to):
        part = half_of(k, whose, half)
        remote(part, part, left_send.at[k], left_recv.at[k, at], l, rep_of(h, to, c))

    def left_start(k):
        left_send_half(k, y, 0, 0, up)
        left_send_half(k, y, 1, 1, down)
        left_send_half(k, y, 1, 2, up)
        left_send_half(k, y, 0, 2, down)
        settle(left.at[k, pl.ds(0, 3)], left_send.at[k])

    def left_forward(k):
        arrive(half_of(k, down, 0), left_recv.at[k, 0])
        left_send_half(k, down, 0, 2, up)
        arrive(half_of(k, up, 1), left_recv.at[k, 1])
        left_send_half(k, up, 1, 2, down)

    def left_ready(k):
        arrive(left.at[k, pl.ds(0, 2)], left_recv.at[k, 2])

    def inside(n):
        row = big + n - 2
        return both(row >= 0, row < 2 * layers)

    def wanted(n, dl):
        return dl != (1 if n == 0 else 3)

    def chunk(k, cd, kk):
        return left.at[k, y, 2 * cd + kk]

    def right_start(k):
        four, eight = left.at[k, y, pl.ds(0, 2)], left.at[k, y]

        def send(at, cd, kk, n, layer, rep, cond=None):
            remote(
                chunk(k, cd, kk), right.at[k, n, c, kk], right_send.at[k, at],
                right_recv.at[k, n, kk], layer, rep, cond,
            )

        for kk in (0, 1):
            for cd in range(2):
                send(0, cd, kk, 1 + 2 * h, l, rep_of(1 - h, y, cd))
        settle(eight, right_send.at[k, 0])
        direct = both(cross, delta != 1 + 2 * h)
        for cd in range(2):
            send(1, cd, 0, 3 - 2 * h, l + over, rep_of(1 - h, y, cd), cross)
            remote(
                chunk(k, cd, 1), stage.at[k, c], right_send.at[k, 1],
                stage_recv.at[k], l - 3 * over, rep_of(h, y, cd), cross,
            )
            send(2, cd, 1, 4 - 4 * h, l + over, rep_of(h, y, cd), direct)
        settle(eight, right_send.at[k, 1], cross)
        settle(four, right_send.at[k, 2], direct)
        for kk in (1, 0):
            use = delta != 3
            up_cond = both(no(edge_up), either(last, use) if kk == 1 else use)
            use = delta != 1
            down_cond = both(no(edge_down), either(first, use) if kk == 1 else use)
            for cd in range(2):
                send(3 + kk, cd, kk, 0, l + 1, rep_of(h, y, cd), up_cond)
                send(5 + kk, cd, kk, 4, l - 1, rep_of(h, y, cd), down_cond)
            settle(four, right_send.at[k, 3 + kk], up_cond)
            settle(four, right_send.at[k, 5 + kk], down_cond)
        remote(
            left.at[k, y, pl.ds(2 * other, 2)], right.at[k, 2, c],
            right_send.at[k, 7], right_recv.at[k, 2, 0], l, rep_of(h, y, other),
        )
        settle(four, right_send.at[k, 7])
        right[k, 2, c] = left[k, y, pl.ds(2 * c, 2)]

    def got_chunk(k, n, kk, cond=None):
        arrive(right.at[k, n, pl.ds(0, 2), kk], right_recv.at[k, n, kk], cond)

    def right_relay(k, parts=(0, 1, 2)):
        four, eight = left.at[k, y, pl.ds(0, 2)], left.at[k, y]
        near = both(cross, delta != 2)
        step = jnp.where(first, 3, 1)
        want = mod(delta + step, 4) != jnp.where(first, 1, 3)

        def hand(at, n_from, n_to, kk, layer, rep, cond):
            for cc in range(2):
                remote(
                    right.at[k, n_from, cc, kk], right.at[k, n_to, cc, kk], right_send.at[k, at],
                    right_recv.at[k, n_to, kk], layer, rep, cond,
                )

        if 0 in parts:
            got_chunk(k, 3 - 2 * h, 0)
            hand(8, 3 - 2 * h, 1 + 2 * h, 0, ahead, rep_of(h, y, c), flat)
            settle(four, right_send.at[k, 8], flat)
            hand(11, 3 - 2 * h, 4 - 4 * h, 0, l + over, rep_of(1 - h, y, c), near)
            got_chunk(k, 1 + 2 * h, 0, cross)
            hand(10, 1 + 2 * h, 4 * h, 0, l, rep_of(1 - h, y, c), both(cross, want))
            settle(four, right_send.at[k, 10], both(cross, want))
        if 1 in parts:
            arrive(stage.at[k], stage_recv.at[k], carry)
            for cc in range(2):
                remote(
                    stage.at[k, cc], right.at[k, 3 - 2 * h, cc, 1], right_send.at[k, 12],
                    right_recv.at[k, 3 - 2 * h, 1], l + 4 * over, rep_of(1 - h, y, c), carry,
                )
            settle(four, right_send.at[k, 12], carry)
            got_chunk(k, 4 - 4 * h, 1, flat)
            hand(9, 4 - 4 * h, 3 - 2 * h, 1, l, rep_of(1 - h, y, c), flat)
            settle(four, right_send.at[k, 9], flat)
        if 2 in parts:
            got_chunk(k, 3 - 2 * h, 1, cross)
            hand(11, 3 - 2 * h, 4 - 4 * h, 1, l + over, rep_of(1 - h, y, c), near)
            settle(eight, right_send.at[k, 11], near)

    def right_ready(k):
        arrive(right.at[k, 2, other], right_recv.at[k, 2, 0])
        low = both(below, delta != 1)
        high = both(above, delta != 3)
        got_chunk(k, 3 - 2 * h, 1, no(cross))
        got_chunk(k, 1 + 2 * h, 0, flat_behind)
        got_chunk(k, 1 + 2 * h, 1, either(flat_behind, cross))
        got_chunk(k, 0, 0, low)
        got_chunk(k, 0, 1, both(low, no(both(last, no(edge_down)))))
        got_chunk(k, 4, 0, high)
        got_chunk(k, 4, 1, both(high, no(both(first, no(edge_up)))))

    nothing = jnp.zeros((t, t), BF)
    apart = delta == 2
    toward = jnp.where(delta == 3, -1, delta)
    middle = (jnp.where(apart, -2, toward), jnp.where(apart, 2, toward))

    def build_left(kl):
        for s in range(2):
            for at, n in enumerate((0, 1, 2) if s == 0 else (2, 3, 4)):
                cls = mod(big + n + 2, 4)
                for kk in range(2):
                    inner = 2 * c + kk
                    for a in range(4):
                        tile = left[kl, cls, a, kk]
                        if n == 0:
                            tile = jnp.where(inner >= a, tile, nothing)
                        if n == 4:
                            tile = jnp.where(inner < a, tile, nothing)
                        lhs[s, a * t:(a + 1) * t, (2 * at + kk) * t:(2 * at + kk + 1) * t] = tile

    def build_right(kr, rows):
        for s in range(2):
            for at, n in enumerate((0, 1, 2) if s == 0 else (2, 3, 4)):
                if n not in rows:
                    continue
                gap = middle[s] - (n - 2)
                for kk in range(2):
                    inner = 2 * c + kk
                    for b in range(4):
                        whole = jnp.logical_and(gap >= -1, gap <= 1)
                        low = jnp.logical_and(gap == 2, b < inner)
                        high = jnp.logical_and(gap == -2, b >= inner)
                        good = jnp.logical_or(whole, jnp.logical_or(low, high))
                        if n != 2:
                            good = both(good, inside(n))
                        if s == 1 and n == 2:
                            good = jnp.logical_and(good, apart)
                        tile = jnp.where(good, right[kr, n, b // 2, kk, b % 2], nothing)
                        rhs[s, b // 2, (2 * at + kk) * t:(2 * at + kk + 1) * t, (b % 2) * t:(b % 2 + 1) * t] = tile

    def columns(half):
        first_out = jnp.dot(lhs[0], rhs[0, half], preferred_element_type=F32)
        second_out = jnp.dot(lhs[1], rhs[1, half], preferred_element_type=F32)

        def value(a, b2):
            b = 2 * half + b2
            use_first = either(no(apart), b >= a)
            use_second = either(no(apart), b < a)
            empty = jnp.zeros((t, t), F32)
            x = first_out[a * t:(a + 1) * t, b2 * t:(b2 + 1) * t]
            z = second_out[a * t:(a + 1) * t, b2 * t:(b2 + 1) * t]
            return jnp.where(use_first, x, empty) + jnp.where(use_second, z, empty)

        return value

    def multiply(k):
        part = columns(other)
        for a in range(4):
            for b2 in range(2):
                give[k, a, b2] = part(a, b2).astype(BF)
        remote(
            give.at[k], got.at[k], pair_send.at[k], pair_recv.at[k], l, rep_of(h, y, other)
        )
        settle(give.at[k], pair_send.at[k])
        part = columns(c)
        for a in range(4):
            for b2 in range(2):
                prod[a, b2] = part(a, b2)

    def summed(k, a, b2):
        value = prod[a, b2] + got[k, a, b2].astype(F32)
        return value

    def marked(a, b2):
        return marks_home[a, b2][0:1, :] == 1

    def owner_send(k, out_ref):
        for a in range(4):
            for b2 in range(2):
                done[k, a, b2] = jnp.where(
                    marked(a, b2), summed(k, a, b2), jnp.zeros((t, t), F32)
                ).astype(BF)
        for a in range(4):
            for b2 in range(2):
                slot = mod(4 * y + 2 * c + b2 + shift - (4 * h + a) + 32, 16)
                here = slot == r
                mine = pltpu.make_async_copy(
                    done.at[k, a, b2], out_ref.at[4 * h + a, 0], self_sem.at[k]
                )
                pl.when(here)(mine.start)
                remote(
                    done.at[k, a, b2], out_ref.at[4 * h + a, 0], out_send.at[k],
                    out_recv.at[k], l, slot, slot != r,
                )
        moved(kept.at[k], out_send.at[k])
        for n in (1, 2):
            mine = pltpu.make_async_copy(
                kept.at[k, pl.ds(0, n)], out_ref.at[pl.ds(0, n), 0], self_sem.at[k]
            )
            kept_here.append((staying == n, mine))

    def owner_ready(k):
        arrived(kept.at[k], out_recv.at[k])

    def marks_ready():
        arrived(marks, mark_recv)

    def finish_u():
        arrive(got.at[U], pair_recv.at[U])
        rows = lax.broadcasted_iota(jnp.int32, (t, t), 0)
        cols = lax.broadcasted_iota(jnp.int32, (t, t), 1)
        for a in range(4):
            for b2 in range(2):
                on = jnp.logical_and(mod(big, 4) == y, 2 * c + b2 == a)
                eye = jnp.where(rows == cols, jnp.where(on, F32(1.5), F32(0.0)), F32(0.0))
                value = eye - 0.5 * summed(U, a, b2)
                left[U, y, a, b2] = jnp.where(marked(a, b2), value, jnp.zeros((t, t), F32)).astype(BF)

    scatter(Y)
    scatter(Z)
    home_ready(Y)
    right_start(Y)
    home_ready(Z)
    left_start(Z)
    right_relay(Y, (0,))
    left_forward(Z)
    right_relay(Y, (1, 2))
    right_start(Z)
    left_start(Y)
    marks_ready()
    left_ready(Z)
    build_left(Z)
    right_ready(Y)
    build_right(Y, (0, 1, 2, 3, 4))
    multiply(U)
    left_forward(Y)
    right_relay(Z)
    finish_u()
    left_start(U)
    right_start(U)
    left_forward(U)
    right_relay(U)
    right_ready(Z)
    build_right(Z, (0, 1, 2, 3, 4))
    left_ready(U)
    build_left(U)
    multiply(Z)
    arrive(got.at[Z], pair_recv.at[Z])
    owner_send(Z, w_out)
    left_ready(Y)
    build_left(Y)
    right_ready(U)
    build_right(U, (0, 1, 2, 3, 4))
    multiply(Y)
    arrive(got.at[Y], pair_recv.at[Y])
    owner_send(Y, x_out)
    owner_ready(Z)
    owner_ready(Y)
    for cond, copy in kept_here:
        pl.when(cond)(copy.wait)
    for cond, copy in pending:
        if cond is None:
            copy.wait_send()
        else:
            pl.when(cond)(copy.wait_send)


def solution(mesh):
    layers = mesh.shape["layer"]

    def body(inverse_root, square_root, pattern):
        t = inverse_root.shape[-1]
        dma = pltpu.SemaphoreType.DMA
        return pl.pallas_call(
            functools.partial(kernel, layers, t),
            out_shape=[
                jax.ShapeDtypeStruct(inverse_root.shape, BF),
                jax.ShapeDtypeStruct(square_root.shape, BF),
            ],
            in_specs=[
                pl.BlockSpec(memory_space=pl.ANY),
                pl.BlockSpec(memory_space=pl.ANY),
                pl.BlockSpec(memory_space=pl.ANY),
            ],
            out_specs=[pl.BlockSpec(memory_space=pl.ANY)] * 2,
            scratch_shapes=[
                pltpu.SMEM((8,), jnp.int32),
                pltpu.VMEM((2, 8, t, t), BF),
                pltpu.VMEM((2, 8, t, t), BF),
                pltpu.VMEM((8, 8, 128), jnp.int32),
                pltpu.VMEM((4, 2, 8, 128), jnp.int32),
                pltpu.VMEM((3, 4, 4, 2, t, t), BF),
                pltpu.VMEM((3, 5, 2, 2, 2, t, t), BF),
                pltpu.VMEM((3, 2, 2, t, t), BF),
                pltpu.VMEM((2, 4 * t, 6 * t), BF),
                pltpu.VMEM((2, 2, 6 * t, 2 * t), BF),
                pltpu.VMEM((4, 2, t, t), F32),
                pltpu.VMEM((3, 4, 2, t, t), BF),
                pltpu.VMEM((3, 4, 2, t, t), BF),
                pltpu.VMEM((2, 4, 2, t, t), BF),
                dma((3,)),
                dma((2,)),
                dma((2,)),
                dma,
                dma,
                dma((3,)),
                dma((3, 3)),
                dma((3, 13)),
                dma((3, 5, 2)),
                dma((3,)),
                dma((3,)),
                dma((3,)),
                dma((2,)),
                dma((2,)),
                dma((2,)),
            ],
            compiler_params=pltpu.CompilerParams(
                collective_id=0, has_side_effects=True, vmem_limit_bytes=67043328
            ),
            name="band_step",
        )(inverse_root, square_root, pattern.reshape(-1))

    return jax.shard_map(
        body,
        mesh=mesh,
        in_specs=(P("layer", "rep", None, None), P("layer", "rep", None, None), P("layer", "rep")),
        out_specs=(P("layer", "rep", None, None), P("layer", "rep", None, None)),
        check_vma=False,
    )
```

```python
import functools

import jax
import jax.numpy as jnp
from jax import lax
from jax.experimental import pallas as pl
from jax.experimental.pallas import tpu as pltpu
from jax.sharding import PartitionSpec as P

BF = jnp.bfloat16
F32 = jnp.float32
MESH = pl.DeviceIdType.MESH
Z, Y, U = 0, 1, 2


def mod(a, b):
    return lax.rem(a, jnp.int32(b))


def div(a, b):
    return lax.div(a, jnp.int32(b))


def kernel(
    layers, t,
    z_hbm, y_hbm, pat_hbm, w_out, x_out,
    pat_ref, raw, kept, marks, marks_home, left, right, stage, lhs, rhs, prod, give, got, done,
    in_sem, home_send, home_recv, mark_send, mark_recv,
    left_send, left_recv, right_send, right_recv, stage_recv, pair_send, pair_recv, out_send, out_recv, self_sem,
):
    l = lax.axis_index("layer")
    r = lax.axis_index("rep")
    h, y, c = div(r, 8), mod(div(r, 2), 4), mod(r, 2)
    big = 2 * l + h
    shift = 8 * mod(l + 1, 2)
    delta = mod(y + 4 * layers * 2 - big, 4)
    other = 1 - c
    pending = []
    kept_here = []

    def rep_of(hh, yy, cc):
        return hh * 8 + yy * 2 + cc

    def remote(src, dst, send_sem, recv_sem, layer, rep, cond=None):
        copy = pltpu.make_async_remote_copy(
            src_ref=src, dst_ref=dst, send_sem=send_sem, recv_sem=recv_sem,
            device_id=(layer, rep), device_id_type=MESH,
        )
        if cond is None:
            copy.start()
        else:
            pl.when(cond)(copy.start)

    def settle(size, send_sem, cond=None):
        copy = pltpu.make_async_remote_copy(
            src_ref=size, dst_ref=size, send_sem=send_sem, recv_sem=send_sem,
            device_id=(l, r), device_id_type=MESH,
        )
        pending.append((cond, copy))

    def arrive(dst, recv_sem, cond=None):
        copy = pltpu.make_async_remote_copy(
            src_ref=dst, dst_ref=dst, send_sem=recv_sem, recv_sem=recv_sem,
            device_id=(l, r), device_id_type=MESH,
        )
        if cond is None:
            copy.wait_recv()
        else:
            pl.when(cond)(copy.wait_recv)

    loads = [
        pltpu.make_async_copy(ref.at[:, 0], raw.at[k], in_sem.at[k])
        for k, ref in ((Z, z_hbm), (Y, y_hbm))
    ]
    pat_load = pltpu.make_async_copy(pat_hbm, pat_ref, in_sem.at[2])
    pat_load.start()
    for load in loads:
        load.start()

    above, below = l < layers - 1, l > 0
    first, last = h == 0, h == 1
    edge_up, edge_down = mod(l, 4) == 3, mod(l, 4) == 0
    both = jnp.logical_and
    either = jnp.logical_or
    no = jnp.logical_not
    ahead = jnp.where(first, l + 1, l - 1)
    over = 2 * h - 1
    flat = no(either(both(first, edge_up), both(last, edge_down)))
    flat_behind = no(either(both(first, edge_down), both(last, edge_up)))
    cross = both(no(flat_behind), either(both(first, below), both(last, above)))
    carry = both(no(flat), either(both(first, l >= 4), both(last, l + 4 < layers)))

    barrier = pltpu.get_barrier_semaphore()
    for step in range(1, 16):
        pl.semaphore_signal(
            barrier, inc=1, device_id=(l, mod(r + step, 16)), device_id_type=MESH
        )
    for near, there in ((l + 1, above), (l - 1, below)):

        @pl.when(there)
        def _():
            for hh in range(2):
                for cc in range(2):
                    pl.semaphore_signal(
                        barrier, inc=1, device_id=(near, rep_of(hh, y, cc)), device_id_type=MESH
                    )


    for role, hop in ((cross, -3), (carry, 3)):

        @pl.when(role)
        def _():
            for cc in range(2):
                for layer, hh in ((l + hop * over, h), (l + 4 * over, 1 - h)):
                    pl.semaphore_signal(
                        barrier, inc=1, device_id=(layer, rep_of(hh, y, cc)), device_id_type=MESH
                    )

    pat_load.wait()
    for ap in range(8):
        marks[ap] = jnp.full((8, 128), pat_ref[ap], jnp.int32)
    for k in (Z, Y):
        loads[k].wait()
        for ap in range(8):
            kept[k, ap] = jnp.where(pat_ref[ap] == 1, raw[k, ap], jnp.zeros((t, t), BF))
    peers = 15 + 4 * sum(x.astype(jnp.int32) for x in (above, below, cross, carry))
    pl.semaphore_wait(barrier, peers)

    def home_of(ap):
        jm = mod(shift + ap + r, 16)
        return div(jm, 4), div(mod(jm, 4), 2), mod(jm, 2)

    def to_rep(ap):
        yd, cd, _ = home_of(ap)
        return rep_of(ap // 4, yd, cd)

    staying = sum((to_rep(ap) == r).astype(jnp.int32) for ap in range(8))

    def moved(ref, sem):
        for n in (6, 7, 8):
            settle(ref.at[pl.ds(0, n)], sem, 8 - staying == n)

    def arrived(ref, sem):
        for n in (6, 7, 8):
            arrive(ref.at[pl.ds(0, n)], sem, 8 - staying == n)

    def scatter(k):
        for ap in (0, 4, 2, 6, 1, 5, 3, 7):
            yd, cd, b2 = home_of(ap)
            dest = rep_of(ap // 4, yd, cd)
            here, away = dest == r, dest != r
            a = ap % 4

            @pl.when(here)
            def _():
                left[k, yd, a, b2] = kept[k, ap]
                if k == Y:
                    marks_home[a, b2] = marks[ap]

            remote(
                kept.at[k, ap], left.at[k, yd, a, b2], home_send.at[k], home_recv.at[k],
                l, dest, away,
            )
            if k == Y:
                remote(
                    marks.at[ap], marks_home.at[a, b2], mark_send, mark_recv, l, dest, away
                )
        moved(kept.at[k], home_send.at[k])
        if k == Y:
            moved(marks, mark_send)

    def home_ready(k):
        arrived(kept.at[k], home_recv.at[k])

    up, down = mod(y + 1, 4), mod(y + 3, 4)
    far = mod(y + 2, 4)

    def half_of(k, whose, half):
        return left.at[k, whose, pl.ds(2 * half, 2)]

    def left_send_half(k, whose, half, at, to):
        part = half_of(k, whose, half)
        remote(part, part, left_send.at[k], left_recv.at[k, at], l, rep_of(h, to, c))

    def left_start(k):
        left_send_half(k, y, 0, 0, up)
        left_send_half(k, y, 1, 1, down)
        left_send_half(k, y, 1, 2, up)
        left_send_half(k, y, 0, 2, down)
        settle(left.at[k, pl.ds(0, 3)], left_send.at[k])

    def left_forward(k):
        arrive(half_of(k, down, 0), left_recv.at[k, 0])
        left_send_half(k, down, 0, 2, up)
        arrive(half_of(k, up, 1), left_recv.at[k, 1])
        left_send_half(k, up, 1, 2, down)

    def left_ready(k):
        arrive(left.at[k, pl.ds(0, 2)], left_recv.at[k, 2])

    def inside(n):
        row = big + n - 2
        return both(row >= 0, row < 2 * layers)

    def wanted(n, dl):
        return dl != (1 if n == 0 else 3)

    def chunk(k, cd, kk):
        return left.at[k, y, 2 * cd + kk]

    def right_start(k):
        four, eight = left.at[k, y, pl.ds(0, 2)], left.at[k, y]

        def send(at, cd, kk, n, layer, rep, cond=None):
            remote(
                chunk(k, cd, kk), right.at[k, n, c, kk], right_send.at[k, at],
                right_recv.at[k, n, kk], layer, rep, cond,
            )

        for kk in (0, 1):
            for cd in range(2):
                send(0, cd, kk, 1 + 2 * h, l, rep_of(1 - h, y, cd))
        settle(eight, right_send.at[k, 0])
        direct = both(cross, delta != 1 + 2 * h)
        for cd in range(2):
            send(1, cd, 0, 3 - 2 * h, l + over, rep_of(1 - h, y, cd), cross)
            remote(
                chunk(k, cd, 1), stage.at[k, c], right_send.at[k, 1],
                stage_recv.at[k], l - 3 * over, rep_of(h, y, cd), cross,
            )
            send(2, cd, 1, 4 - 4 * h, l + over, rep_of(h, y, cd), direct)
        settle(eight, right_send.at[k, 1], cross)
        settle(four, right_send.at[k, 2], direct)
        for kk in (1, 0):
            use = delta != 3
            up_cond = both(no(edge_up), either(last, use) if kk == 1 else use)
            use = delta != 1
            down_cond = both(no(edge_down), either(first, use) if kk == 1 else use)
            for cd in range(2):
                send(3 + kk, cd, kk, 0, l + 1, rep_of(h, y, cd), up_cond)
                send(5 + kk, cd, kk, 4, l - 1, rep_of(h, y, cd), down_cond)
            settle(four, right_send.at[k, 3 + kk], up_cond)
            settle(four, right_send.at[k, 5 + kk], down_cond)
        remote(
            left.at[k, y, pl.ds(2 * other, 2)], right.at[k, 2, c],
            right_send.at[k, 7], right_recv.at[k, 2, 0], l, rep_of(h, y, other),
        )
        settle(four, right_send.at[k, 7])
        right[k, 2, c] = left[k, y, pl.ds(2 * c, 2)]

    def got_chunk(k, n, kk, cond=None):
        arrive(right.at[k, n, pl.ds(0, 2), kk], right_recv.at[k, n, kk], cond)

    def right_relay(k, parts=(0, 1, 2)):
        four, eight = left.at[k, y, pl.ds(0, 2)], left.at[k, y]
        near = both(cross, delta != 2)
        step = jnp.where(first, 3, 1)
        want = mod(delta + step, 4) != jnp.where(first, 1, 3)

        def hand(at, n_from, n_to, kk, layer, rep, cond):
            for cc in range(2):
                remote(
                    right.at[k, n_from, cc, kk], right.at[k, n_to, cc, kk], right_send.at[k, at],
                    right_recv.at[k, n_to, kk], layer, rep, cond,
                )

        if 0 in parts:
            got_chunk(k, 3 - 2 * h, 0)
            hand(8, 3 - 2 * h, 1 + 2 * h, 0, ahead, rep_of(h, y, c), flat)
            settle(four, right_send.at[k, 8], flat)
            hand(11, 3 - 2 * h, 4 - 4 * h, 0, l + over, rep_of(1 - h, y, c), near)
            got_chunk(k, 1 + 2 * h, 0, cross)
            hand(10, 1 + 2 * h, 4 * h, 0, l, rep_of(1 - h, y, c), both(cross, want))
            settle(four, right_send.at[k, 10], both(cross, want))
        if 1 in parts:
            arrive(stage.at[k], stage_recv.at[k], carry)
            for cc in range(2):
                remote(
                    stage.at[k, cc], right.at[k, 3 - 2 * h, cc, 1], right_send.at[k, 12],
                    right_recv.at[k, 3 - 2 * h, 1], l + 4 * over, rep_of(1 - h, y, c), carry,
                )
            settle(four, right_send.at[k, 12], carry)
            got_chunk(k, 4 - 4 * h, 1, flat)
            hand(9, 4 - 4 * h, 3 - 2 * h, 1, l, rep_of(1 - h, y, c), flat)
            settle(four, right_send.at[k, 9], flat)
        if 2 in parts:
            got_chunk(k, 3 - 2 * h, 1, cross)
            hand(11, 3 - 2 * h, 4 - 4 * h, 1, l + over, rep_of(1 - h, y, c), near)
            settle(eight, right_send.at[k, 11], near)

    def right_ready(k):
        arrive(right.at[k, 2, other], right_recv.at[k, 2, 0])
        low = both(below, delta != 1)
        high = both(above, delta != 3)
        got_chunk(k, 3 - 2 * h, 1, no(cross))
        got_chunk(k, 1 + 2 * h, 0, flat_behind)
        got_chunk(k, 1 + 2 * h, 1, either(flat_behind, cross))
        got_chunk(k, 0, 0, low)
        got_chunk(k, 0, 1, both(low, no(both(last, no(edge_down)))))
        got_chunk(k, 4, 0, high)
        got_chunk(k, 4, 1, both(high, no(both(first, no(edge_up)))))

    nothing = jnp.zeros((t, t), BF)
    apart = delta == 2
    toward = jnp.where(delta == 3, -1, delta)
    middle = (jnp.where(apart, -2, toward), jnp.where(apart, 2, toward))

    def build_left(kl):
        for s in range(2):
            for at, n in enumerate((0, 1, 2) if s == 0 else (2, 3, 4)):
                cls = mod(big + n + 2, 4)
                for kk in range(2):
                    inner = 2 * c + kk
                    for a in range(4):
                        tile = left[kl, cls, a, kk]
                        if n == 0:
                            tile = jnp.where(inner >= a, tile, nothing)
                        if n == 4:
                            tile = jnp.where(inner < a, tile, nothing)
                        lhs[s, a * t:(a + 1) * t, (2 * at + kk) * t:(2 * at + kk + 1) * t] = tile

    def build_right(kr, rows):
        for s in range(2):
            for at, n in enumerate((0, 1, 2) if s == 0 else (2, 3, 4)):
                if n not in rows:
                    continue
                gap = middle[s] - (n - 2)
                for kk in range(2):
                    inner = 2 * c + kk
                    for b in range(4):
                        whole = jnp.logical_and(gap >= -1, gap <= 1)
                        low = jnp.logical_and(gap == 2, b < inner)
                        high = jnp.logical_and(gap == -2, b >= inner)
                        good = jnp.logical_or(whole, jnp.logical_or(low, high))
                        if n != 2:
                            good = both(good, inside(n))
                        if s == 1 and n == 2:
                            good = jnp.logical_and(good, apart)
                        tile = jnp.where(good, right[kr, n, b // 2, kk, b % 2], nothing)
                        rhs[s, b // 2, (2 * at + kk) * t:(2 * at + kk + 1) * t, (b % 2) * t:(b % 2 + 1) * t] = tile

    def columns(half):
        first_out = jnp.dot(lhs[0], rhs[0, half], preferred_element_type=F32)
        second_out = jnp.dot(lhs[1], rhs[1, half], preferred_element_type=F32)

        def value(a, b2):
            b = 2 * half + b2
            use_first = either(no(apart), b >= a)
            use_second = either(no(apart), b < a)
            empty = jnp.zeros((t, t), F32)
            x = first_out[a * t:(a + 1) * t, b2 * t:(b2 + 1) * t]
            z = second_out[a * t:(a + 1) * t, b2 * t:(b2 + 1) * t]
            return jnp.where(use_first, x, empty) + jnp.where(use_second, z, empty)

        return value

    def multiply(k):
        part = columns(other)
        for a in range(4):
            for b2 in range(2):
                give[k, a, b2] = part(a, b2).astype(BF)
        remote(
            give.at[k], got.at[k], pair_send.at[k], pair_recv.at[k], l, rep_of(h, y, other)
        )
        settle(give.at[k], pair_send.at[k])
        part = columns(c)
        for a in range(4):
            for b2 in range(2):
                prod[a, b2] = part(a, b2)

    def summed(k, a, b2):
        value = prod[a, b2] + got[k, a, b2].astype(F32)
        return value

    def marked(a, b2):
        return marks_home[a, b2][0:1, :] == 1

    def owner_send(k, out_ref):
        def finish(a, b2):
            done[k, a, b2] = jnp.where(
                marked(a, b2), summed(k, a, b2), jnp.zeros((t, t), F32)
            ).astype(BF)

        finish(0, 0)
        finish(0, 1)
        for a in range(4):
            for b2 in range(2):
                after = 2 * a + b2 + 2
                if after < 8:
                    finish(after // 2, after % 2)
                slot = mod(4 * y + 2 * c + b2 + shift - (4 * h + a) + 32, 16)
                here = slot == r
                mine = pltpu.make_async_copy(
                    done.at[k, a, b2], out_ref.at[4 * h + a, 0], self_sem.at[k]
                )
                pl.when(here)(mine.start)
                remote(
                    done.at[k, a, b2], out_ref.at[4 * h + a, 0], out_send.at[k],
                    out_recv.at[k], l, slot, slot != r,
                )
        moved(kept.at[k], out_send.at[k])
        for n in (1, 2):
            mine = pltpu.make_async_copy(
                kept.at[k, pl.ds(0, n)], out_ref.at[pl.ds(0, n), 0], self_sem.at[k]
            )
            kept_here.append((staying == n, mine))

    def owner_ready(k):
        arrived(kept.at[k], out_recv.at[k])

    def marks_ready():
        arrived(marks, mark_recv)

    def finish_u():
        arrive(got.at[U], pair_recv.at[U])
        rows = lax.broadcasted_iota(jnp.int32, (t, t), 0)
        cols = lax.broadcasted_iota(jnp.int32, (t, t), 1)
        for a in range(4):
            for b2 in range(2):
                on = jnp.logical_and(mod(big, 4) == y, 2 * c + b2 == a)
                eye = jnp.where(rows == cols, jnp.where(on, F32(1.5), F32(0.0)), F32(0.0))
                value = eye - 0.5 * summed(U, a, b2)
                left[U, y, a, b2] = jnp.where(marked(a, b2), value, jnp.zeros((t, t), F32)).astype(BF)

    scatter(Y)
    scatter(Z)
    home_ready(Y)
    right_start(Y)
    home_ready(Z)
    left_start(Z)
    right_relay(Y, (0,))
    left_forward(Z)
    right_relay(Y, (1, 2))
    right_start(Z)
    left_start(Y)
    marks_ready()
    left_ready(Z)
    build_left(Z)
    right_ready(Y)
    build_right(Y, (0, 1, 2, 3, 4))
    multiply(U)
    left_forward(Y)
    right_relay(Z)
    finish_u()
    left_start(U)
    right_start(U)
    left_forward(U)
    right_relay(U)
    right_ready(Z)
    build_right(Z, (0, 1, 2, 3, 4))
    left_ready(U)
    build_left(U)
    multiply(Z)
    arrive(got.at[Z], pair_recv.at[Z])
    owner_send(Z, w_out)
    left_ready(Y)
    build_left(Y)
    right_ready(U)
    build_right(U, (0, 1, 2, 3, 4))
    multiply(Y)
    arrive(got.at[Y], pair_recv.at[Y])
    owner_send(Y, x_out)
    owner_ready(Z)
    owner_ready(Y)
    for cond, copy in kept_here:
        pl.when(cond)(copy.wait)
    for cond, copy in pending:
        if cond is None:
            copy.wait_send()
        else:
            pl.when(cond)(copy.wait_send)


def solution(mesh):
    layers = mesh.shape["layer"]

    def body(inverse_root, square_root, pattern):
        t = inverse_root.shape[-1]
        dma = pltpu.SemaphoreType.DMA
        return pl.pallas_call(
            functools.partial(kernel, layers, t),
            out_shape=[
                jax.ShapeDtypeStruct(inverse_root.shape, BF),
                jax.ShapeDtypeStruct(square_root.shape, BF),
            ],
            in_specs=[
                pl.BlockSpec(memory_space=pl.ANY),
                pl.BlockSpec(memory_space=pl.ANY),
                pl.BlockSpec(memory_space=pl.ANY),
            ],
            out_specs=[pl.BlockSpec(memory_space=pl.ANY)] * 2,
            scratch_shapes=[
                pltpu.SMEM((8,), jnp.int32),
                pltpu.VMEM((2, 8, t, t), BF),
                pltpu.VMEM((2, 8, t, t), BF),
                pltpu.VMEM((8, 8, 128), jnp.int32),
                pltpu.VMEM((4, 2, 8, 128), jnp.int32),
                pltpu.VMEM((3, 4, 4, 2, t, t), BF),
                pltpu.VMEM((3, 5, 2, 2, 2, t, t), BF),
                pltpu.VMEM((3, 2, 2, t, t), BF),
                pltpu.VMEM((2, 4 * t, 6 * t), BF),
                pltpu.VMEM((2, 2, 6 * t, 2 * t), BF),
                pltpu.VMEM((4, 2, t, t), F32),
                pltpu.VMEM((3, 4, 2, t, t), BF),
                pltpu.VMEM((3, 4, 2, t, t), BF),
                pltpu.VMEM((2, 4, 2, t, t), BF),
                dma((3,)),
                dma((2,)),
                dma((2,)),
                dma,
                dma,
                dma((3,)),
                dma((3, 3)),
                dma((3, 13)),
                dma((3, 5, 2)),
                dma((3,)),
                dma((3,)),
                dma((3,)),
                dma((2,)),
                dma((2,)),
                dma((2,)),
            ],
            compiler_params=pltpu.CompilerParams(
                collective_id=0, has_side_effects=True, vmem_limit_bytes=67043328
            ),
            name="band_step",
        )(inverse_root, square_root, pattern.reshape(-1))

    return jax.shard_map(
        body,
        mesh=mesh,
        in_specs=(P("layer", "rep", None, None), P("layer", "rep", None, None), P("layer", "rep")),
        out_specs=(P("layer", "rep", None, None), P("layer", "rep", None, None)),
        check_vma=False,
    )
```
